128 devices in a mesh: seq: 32 (over z, y, x_lo), tp: 2 (over core), pp: 2 (over x_hi).
Axes of the slice: x: 4 (x_hi: 2, x_lo: 2; x = x_hi * 2 + x_lo), y: 4, z: 4, core: 2. Of those that a mesh axis runs over, the one named last changes fastest.
Arguments:
- queries: bfloat16 [2, 16384, 4096], P('pp', 'seq', 'tp'), may hold values from -1.796875 to 1.796875
- keys: bfloat16 [2, 16384, 4096], P('pp', 'seq', 'tp'), may hold values from -1.796875 to 1.796875
- values: bfloat16 [2, 16384, 4096], P('pp', 'seq', 'tp'), may hold values from -25.375 to 25.375
- upstream: bfloat16 [2, 16384, 3072], P('pp', 'seq', 'tp'), may hold values from -6 to 6
- out_weight: bfloat16 [2, 4096, 3072], P('pp', 'tp'), may hold values from -0.09375 to 0.09375
- gain: float32 [2, 4096], P('pp', 'tp'), may hold values from 0.25 to 1.75
- log_decay: float32 [2, 32, 16384], P('pp', 'tp', 'seq'), may hold values from -0.7 to 0
Outputs:
- grad_queries: bfloat16 [2, 16384, 4096], P('pp', 'seq', 'tp')
- grad_keys: bfloat16 [2, 16384, 4096], P('pp', 'seq', 'tp')
- grad_values: bfloat16 [2, 16384, 4096], P('pp', 'seq', 'tp')
The draws below stay inside these ranges and needn't reach their ends.
All inputs are finite; a program needn't handle non-finite values.
Results may differ from the reference program's by a relative error of at most 0.014.
Values may be sent and summed in bfloat16 or wider, within the bound.
A program may use at most 128 MiB of HBM per device.

```python
import math
import jax
import jax.numpy as jnp
from jax import lax

D = 3072
HEADS = 32
HEAD = 128
TOK_DEV = 512
SECTIONS = 2
SEQUENCE_SLOTS = 16384
FEATURES = 4096


def draw_log_decay(key, part):
    sampler_keychain = jax.random.split(key, 10)
    fast_share = 0.25
    block_count = SEQUENCE_SLOTS // TOK_DEV
    is_fast = jax.random.uniform(sampler_keychain[0], (SECTIONS, HEADS)) < fast_share
    has_reset = jnp.logical_and(jax.random.uniform(sampler_keychain[7], (SECTIONS, HEADS)) < 0.3, jnp.logical_not(is_fast))
    fast_rate = jnp.exp(jax.random.uniform(sampler_keychain[1], (SECTIONS, HEADS), minval=math.log(1.0 / 50.0), maxval=math.log(1.0 / 20.0)))
    slow_rate = jnp.exp(jax.random.uniform(sampler_keychain[2], (SECTIONS, HEADS), minval=math.log(0.1), maxval=math.log(0.5))) / SEQUENCE_SLOTS
    base_rate = jnp.where(is_fast, fast_rate, slow_rate)
    device_factor = jnp.exp(jax.random.uniform(sampler_keychain[3], (SECTIONS, HEADS, block_count), minval=math.log(0.5), maxval=math.log(1.5)))
    device_factor = jnp.repeat(device_factor, TOK_DEV, axis=2)
    token_factor = jax.random.uniform(sampler_keychain[4], (SECTIONS, HEADS, SEQUENCE_SLOTS), minval=0.5, maxval=1.5)
    clustered_index_list = jax.random.randint(sampler_keychain[5], (3,), 0, SEQUENCE_SLOTS)
    objective_numbers = jax.random.uniform(sampler_keychain[6], (SECTIONS, HEADS, 3), minval=0.2, maxval=0.4)
    complete_index_list = jnp.arange(SEQUENCE_SLOTS, dtype=jnp.int32)
    index_tally = complete_index_list[None, None, None, :] == clustered_index_list[None, None, :, None]
    element_cluster = jnp.sum(jnp.where(index_tally, -jnp.log(1.0 - objective_numbers)[:, :, :, None], 0.0), axis=2)
    reset_block = jax.random.randint(sampler_keychain[8], (SECTIONS, HEADS), block_count // 4, block_count - block_count // 4)
    position_block = complete_index_list // TOK_DEV
    position_offset = complete_index_list % TOK_DEV
    in_block = position_block[None, None, :] == reset_block[:, :, None]
    near_end = (position_offset >= TOK_DEV - 6)[None, None, :]
    in_reset = jnp.logical_and(jnp.logical_and(in_block, near_end), has_reset[:, :, None])
    reset_rate = jax.random.uniform(sampler_keychain[9], (SECTIONS, HEADS, SEQUENCE_SLOTS), minval=0.505, maxval=0.55)
    fading_factors = base_rate[:, :, None] * device_factor * token_factor
    total_rate = fading_factors + element_cluster + jnp.where(in_reset, reset_rate, 0.0)
    return (-jnp.minimum(total_rate, 0.7)).astype(jnp.float32)


def draw_values(key, part):
    first_key, second_key, third_key = jax.random.split(key, 3)
    head_place = (jnp.arange(HEADS, dtype=jnp.float32)[None, :] + jax.random.uniform(first_key, (SECTIONS, HEADS))) / HEADS
    head_scale = jnp.exp(math.log(10.0) * (head_place - 0.5))
    feature_scale = jnp.repeat(head_scale, HEAD, axis=1)
    base_draw = jnp.clip(jax.random.normal(second_key, (SECTIONS, SEQUENCE_SLOTS, FEATURES)), -4.0, 4.0)
    token_scale = jnp.exp(jax.random.uniform(third_key, (SECTIONS, SEQUENCE_SLOTS), minval=math.log(0.5), maxval=math.log(2.0)))
    return (base_draw * feature_scale[:, None, :] * token_scale[:, :, None]).astype(jnp.bfloat16)


def steps_of(own_key, shape, pieces, smallest, top_value):
    level, own = 1.0, jax.random.fold_in(own_key, 6)
    for position, shards_of in pieces:
        heights = jnp.exp(jax.random.uniform(jax.random.fold_in(own, position), (shards_of,), jnp.float32, smallest / len(pieces), top_value / len(pieces)))
        level = level * jnp.repeat(heights, shape[position] // shards_of).reshape([-1 if axis == position else 1 for axis in range(len(shape))])
    return level


def scatter_about(stream_key, dims, deviation, reach, shards=(), kind=jnp.bfloat16):
    array = jax.random.normal(stream_key, dims, jnp.float32) * deviation
    if len(shards) > 0:
        array = steps_of(stream_key, dims, shards, -0.22, 0.18) * array
    return jnp.clip(array, min=-reach, max=reach).astype(kind)


def setup_inputs(seed: int = 0) -> dict:
    splits = jax.random.split(jax.random.key(seed), 8)
    return {
        "queries": scatter_about(splits[0], (SECTIONS, SEQUENCE_SLOTS, FEATURES), 0.3, 1.796875, ((0, 2), (1, 32), (2, 2))),
        "keys": scatter_about(splits[1], (SECTIONS, SEQUENCE_SLOTS, FEATURES), 0.3, 1.796875, ((0, 2), (1, 32), (2, 2))),
        "values": draw_values(jax.random.fold_in(splits[7], 71), 0),
        "upstream": scatter_about(splits[3], (SECTIONS, SEQUENCE_SLOTS, D), 1.0, 6.0, ((0, 2), (1, 32), (2, 2))),
        "out_weight": scatter_about(splits[4], (SECTIONS, FEATURES, D), FEATURES ** -0.5, 0.09375, ((0, 2), (1, 2))),
        "gain": jnp.clip(1.0 + 0.15 * jax.random.normal(splits[5], (SECTIONS, FEATURES), jnp.float32), 0.25, 1.75),
        "log_decay": draw_log_decay(jax.random.fold_in(splits[7], 71), 0),
    }


EPS = 1e-06

def mixed(form, left, right):
    return jnp.einsum(form, left.astype(jnp.float32), right.astype(jnp.float32), precision=lax.Precision.HIGHEST)

def decay_matrix(cumulative):
    length = cumulative.shape[1]
    row_ids = lax.broadcasted_iota(jnp.int32, (length, length), 0)
    col_ids = lax.broadcasted_iota(jnp.int32, (length, length), 1)
    causal = (row_ids >= col_ids)[None]
    spread = cumulative[:, :, None] - cumulative[:, None, :]
    return jnp.where(causal, jnp.exp(jnp.where(causal, spread, jnp.float32(0.0))), jnp.float32(0.0))

def make_state(inputs):
    key_rows, value_rows, cumulative, block_total = inputs
    tail_decay = jnp.exp(block_total[:, None] - cumulative).T
    weighted_keys = (key_rows * tail_decay[:, :, None]).astype(jnp.bfloat16)
    return mixed('thd,the->hde', weighted_keys, value_rows)

def attend(inputs):
    query_rows, key_rows, value_rows, cumulative, state_bf = inputs
    masked = (mixed('thd,shd->hts', query_rows, key_rows) * decay_matrix(cumulative)).astype(jnp.bfloat16)
    head_decay = jnp.exp(cumulative).T
    return mixed('hts,shd->thd', masked, value_rows) + head_decay[:, :, None] * mixed('thd,hde->the', query_rows, state_bf)

def make_pass(inputs):
    query_rows, grad_attn, cumulative = inputs
    weighted_queries = (query_rows * jnp.exp(cumulative).T[:, :, None]).astype(jnp.bfloat16)
    return mixed('thd,the->hde', weighted_queries, grad_attn)

def chain_step(state, inputs):
    block_total, local_state = inputs
    return (jnp.exp(block_total)[:, None, None] * state + local_state, state)

def gradients(inputs):
    query_rows, key_rows, value_rows, grad_attn, cumulative, block_total, state_bf, later_bf = inputs
    decay_mat = decay_matrix(cumulative)
    masked = (mixed('thd,shd->hts', query_rows, key_rows) * decay_mat).astype(jnp.bfloat16)
    dmask = (mixed('thd,shd->hts', grad_attn, value_rows) * decay_mat).astype(jnp.bfloat16)
    head_decay = jnp.exp(cumulative).T
    tail_decay = jnp.exp(block_total[:, None] - cumulative).T
    grad_q = mixed('hts,shd->thd', dmask, key_rows) + head_decay[:, :, None] * mixed('the,hde->thd', grad_attn, state_bf)
    grad_k = mixed('hts,thd->shd', dmask, query_rows) + tail_decay[:, :, None] * mixed('the,hde->thd', value_rows, later_bf)
    grad_v = mixed('hts,thd->shd', masked, grad_attn) + tail_decay[:, :, None] * mixed('thd,hde->the', key_rows, later_bf)
    return (grad_q.astype(jnp.bfloat16), grad_k.astype(jnp.bfloat16), grad_v.astype(jnp.bfloat16))

def reference(queries, keys, values, upstream, out_weight, gain, log_decay):
    block_count = SEQUENCE_SLOTS // TOK_DEV
    list_q, list_k, list_v = ([], [], [])
    for section_index in range(SECTIONS):
        grad_out = upstream[(section_index + 1) % SECTIONS]
        query_blocks = queries[section_index].reshape(block_count, TOK_DEV, HEADS, HEAD)
        key_blocks = keys[section_index].reshape(block_count, TOK_DEV, HEADS, HEAD)
        value_blocks = values[section_index].reshape(block_count, TOK_DEV, HEADS, HEAD)
        rate_blocks = log_decay[section_index].reshape(HEADS, block_count, TOK_DEV).transpose(1, 0, 2)
        cumulative = jnp.cumsum(rate_blocks, axis=2)
        block_total = cumulative[:, :, -1]
        local_state = lax.map(make_state, (key_blocks, value_blocks, cumulative, block_total))
        zero_state = jnp.zeros((HEADS, HEAD, HEAD), jnp.float32)
        unused, state_in = lax.scan(chain_step, zero_state, (block_total, local_state))
        state_bf = state_in.astype(jnp.bfloat16)
        attended = lax.map(attend, (query_blocks, key_blocks, value_blocks, cumulative, state_bf))
        flat_out = attended.reshape(SEQUENCE_SLOTS, FEATURES)
        grad_hidden = jnp.dot(grad_out, out_weight[section_index].T, preferred_element_type=jnp.float32)
        inverse = 1.0 / jnp.sqrt(lax.optimization_barrier(jnp.mean(flat_out * flat_out, axis=1)) + EPS)
        grad_norm = grad_hidden * gain[section_index][None, :]
        cross = lax.optimization_barrier(jnp.mean(grad_norm * flat_out, axis=1))
        grad_attn = (inverse[:, None] * grad_norm - (inverse * inverse * inverse * cross)[:, None] * flat_out).astype(jnp.bfloat16)
        grad_blocks = grad_attn.reshape(block_count, TOK_DEV, HEADS, HEAD)
        passed = lax.map(make_pass, (query_blocks, grad_blocks, cumulative))
        unused_two, later_state = lax.scan(chain_step, zero_state, (block_total, passed), reverse=True)
        shifted_total = jnp.concatenate([block_total[1:], jnp.zeros((1, HEADS), jnp.float32)], axis=0)
        shifted_pass = jnp.concatenate([passed[1:], jnp.zeros((1, HEADS, HEAD, HEAD), jnp.float32)], axis=0)
        unused_three, later_state = lax.scan(chain_step, zero_state, (shifted_total, shifted_pass), reverse=True)
        later_state = jnp.exp(shifted_total)[:, :, None, None] * later_state + shifted_pass
        later_bf = later_state.astype(jnp.bfloat16)
        grad_q, grad_k, grad_v = lax.map(gradients, (query_blocks, key_blocks, value_blocks, grad_blocks, cumulative, block_total, state_bf, later_bf))
        list_q.append(grad_q.reshape(SEQUENCE_SLOTS, FEATURES))
        list_k.append(grad_k.reshape(SEQUENCE_SLOTS, FEATURES))
        list_v.append(grad_v.reshape(SEQUENCE_SLOTS, FEATURES))
    return (jnp.stack(list_q), jnp.stack(list_k), jnp.stack(list_v))
```

```python
import jax
import jax.numpy as jnp
from jax import lax
from jax.experimental import pallas as pl
from jax.experimental.pallas import tpu as pltpu
from jax.sharding import Mesh
from jax.sharding import PartitionSpec as P

HEAD = 128
SEQ = ("seq_0", "seq_1", "seq_2")
MESH = pl.DeviceIdType.MESH
EPS = 1e-06
BF = jnp.bfloat16
F32 = jnp.float32

TOK = 512
HALF = 256
WIDTH = 2048
HEADS = 16
MODEL = 3072
CHUNKS = 6
CW = 256
BLOCKS = 32
ROWS = 64
FEATURES = 4096


def nn(a, b):
    return lax.dot_general(a, b, (((1,), (0,)), ((), ())), preferred_element_type=F32)


def nt(a, b):
    return lax.dot_general(a, b, (((1,), (1,)), ((), ())), preferred_element_type=F32)


def lanes(h):
    return pl.ds(pl.multiple_of(h * HEAD, HEAD), HEAD)


def kernel(
    q_hbm, k_hbm, v_hbm, up_hbm, w_hbm, gain_hbm, ld_hbm,
    dq_hbm, dk_hbm, dv_hbm,
    q, k, v, w, up, att, gh, ga, wqt, ccol, crow, mta, mtb,
    own_f, got_f, scan_f, state, own_b, got_b, scan_b, later,
    totals, tot_in, sq_own, sq_in, cr_own, cr_in, inv, fac, gain, ld,
    dqs, dks, dvs,
    load_sem, tot_sem, a2a_sem, perm_send, perm_recv, fwd_send, fwd_recv, tp_sem, out_sem,
):
    z, y, x = (lax.axis_index(a) for a in SEQ)
    me = z * 8 + y * 2 + x
    tp = lax.axis_index("tp")
    sibling = {"tp": 1 - tp}
    across = {"pp": 1 - lax.axis_index("pp")}

    def peer(i):
        p = lax.rem(me + i, BLOCKS)
        return p, {"seq_0": p // 8, "seq_1": lax.rem(p // 2, 4), "seq_2": lax.rem(p, 2)}

    loads = []

    def load(src, dst):
        copy = pltpu.make_async_copy(src, dst, load_sem.at[len(loads)])
        copy.start()
        loads.append(copy)
        return copy

    ld_load = load(ld_hbm.at[0], ld)
    k_load = load(k_hbm.at[0], k)
    v_load = load(v_hbm.at[0], v)
    q_load = load(q_hbm.at[0], q)
    gain_load = load(gain_hbm, gain)
    w_loads = []
    for j in range(CHUNKS):
        for part, side in enumerate((tp, 1 - tp)):
            at = pl.multiple_of(side * (MODEL // 2) + j * CW, CW)
            w_loads.append(
                load(w_hbm.at[0, :, pl.ds(at, CW)], w.at[:, pl.ds((2 * j + part) * CW, CW)])
            )

    barrier = pltpu.get_barrier_semaphore()

    @pl.loop(1, BLOCKS)
    def _(i):
        _, device = peer(i)
        pl.semaphore_signal(barrier, inc=1, device_id=device, device_id_type=MESH)

    pl.semaphore_signal(barrier, inc=1, device_id=sibling, device_id_type=MESH)
    pl.semaphore_signal(barrier, inc=1, device_id=across, device_id_type=MESH)
    pl.semaphore_wait(barrier, BLOCKS + 1)

    def permute(j):
        return pltpu.make_async_remote_copy(
            src_ref=up_hbm.at[0, :, pl.ds(j * CW, CW)],
            dst_ref=up.at[:, pl.ds(2 * j * CW, CW)],
            send_sem=perm_send.at[j],
            recv_sem=perm_recv.at[j],
            device_id=across,
            device_id_type=MESH,
        )

    def forward(j):
        return pltpu.make_async_remote_copy(
            src_ref=up.at[:, pl.ds(2 * j * CW, CW)],
            dst_ref=up.at[:, pl.ds((2 * j + 1) * CW, CW)],
            send_sem=fwd_send.at[j],
            recv_sem=fwd_recv.at[j],
            device_id=sibling,
            device_id_type=MESH,
        )

    def exchange(src, dst, send_sem, recv_sem):
        @pl.loop(1, BLOCKS)
        def _(i):
            p, device = peer(i)
            pltpu.make_async_remote_copy(
                src_ref=src.at[p],
                dst_ref=dst.at[me],
                send_sem=send_sem,
                recv_sem=recv_sem,
                device_id=device,
                device_id_type=MESH,
            ).start()

        dst[me] = src[me]

    def arrived(ref, sem):
        whole = ref.at[pl.ds(0, BLOCKS - 1)]
        pltpu.make_async_copy(whole, whole, sem).wait()

    for j in (0, 1):
        permute(j).start()

    ld_load.wait()
    cum = ld[...]
    place = lax.broadcasted_iota(jnp.int32, (HEADS, TOK), 1)
    step = 1
    while step < TOK:
        moved = pltpu.roll(cum, step, 1)
        cum = cum + jnp.where(place >= step, moved, 0.0)
        step *= 2
    crow[...] = cum
    total = jnp.broadcast_to(cum[:, TOK - 1 : TOK], (HEADS, HEAD))
    for h in range(HEADS):
        totals[2 * h : 2 * h + 1, 0] = total[h : h + 1]
        totals[2 * h + 1 : 2 * h + 2, 0] = total[h : h + 1]
    exchange(totals, tot_in, tot_sem.at[0], tot_sem.at[1])
    turned = cum.T
    for h in range(HEADS):
        ccol[h] = jnp.broadcast_to(turned[:, h : h + 1], (TOK, HEAD))

    k_load.wait()
    v_load.wait()

    @pl.loop(0, HEADS)
    def _(h):
        tail = jnp.exp(totals[2 * h] - ccol[h])
        weighted = (k[:, lanes(h)].astype(F32) * tail).astype(BF)
        local_state = nn(weighted.T, v[:, lanes(h)]).astype(BF)
        own_f[2 * h] = local_state[:ROWS]
        own_f[2 * h + 1] = local_state[ROWS:]

    exchange(own_f, got_f, a2a_sem.at[0], a2a_sem.at[1])
    for j in (2, 3):
        permute(j).start()
    q_load.wait()

    lower = lax.broadcasted_iota(jnp.int32, (HALF, HALF), 0) >= lax.broadcasted_iota(
        jnp.int32, (HALF, HALF), 1
    )
    upper = lax.broadcasted_iota(jnp.int32, (HALF, HALF), 0) <= lax.broadcasted_iota(
        jnp.int32, (HALF, HALF), 1
    )
    low = -1e30

    def decay_parts(h):
        col = ccol[h]
        col2 = jnp.concatenate([col, col], axis=1)
        row = crow[pl.ds(h, 1), :]
        c0, c1 = col2[:HALF], col2[HALF:]
        r0, r1 = row[:, :HALF], row[:, HALF:]
        d00 = jnp.exp(jnp.where(lower, c0 - r0, low))
        d10 = jnp.exp(c1 - r0)
        d11 = jnp.exp(jnp.where(lower, c1 - r1, low))
        return d00, d10, d11

    def turned_parts(h):
        col = ccol[h]
        col2 = jnp.concatenate([col, col], axis=1)
        row = crow[pl.ds(h, 1), :]
        c0, c1 = col2[:HALF], col2[HALF:]
        r0, r1 = row[:, :HALF], row[:, HALF:]
        t00 = jnp.exp(jnp.where(upper, r0 - c0, low))
        t01 = jnp.exp(r1 - c0)
        t11 = jnp.exp(jnp.where(upper, r1 - c1, low))
        return t00, t01, t11

    @pl.loop(0, HEADS)
    def _(h):
        qh, kh, vh = q[:, lanes(h)], k[:, lanes(h)], v[:, lanes(h)]
        q0, q1, k0, k1 = qh[:HALF], qh[HALF:], kh[:HALF], kh[HALF:]
        d00, d10, d11 = decay_parts(h)
        m00 = (nt(q0, k0) * d00).astype(BF)
        m10 = (nt(q1, k0) * d10).astype(BF)
        m11 = (nt(q1, k1) * d11).astype(BF)
        att[:HALF, lanes(h)] = nn(m00, vh[:HALF])
        att[HALF:, lanes(h)] = nn(jnp.concatenate([m10, m11], axis=1), vh)
        t00, t01, t11 = turned_parts(h)
        mta[h, :, :HALF] = (nt(k0, q0) * t00).astype(BF)
        mta[h, :, HALF:] = (nt(k0, q1) * t01).astype(BF)
        mtb[h] = (nt(k1, q1) * t11).astype(BF)
        wq = (qh.astype(F32) * jnp.exp(ccol[h])).astype(BF)
        wqt[h] = wq.T

    arrived(tot_in, tot_sem.at[1])
    arrived(got_f, a2a_sem.at[1])
    running = jnp.zeros((ROWS, HEAD), F32)
    for b in range(BLOCKS):
        scan_f[b] = running.astype(BF)
        running = jnp.exp(tot_in[b]) * running + got_f[b].astype(F32)
    exchange(scan_f, state, a2a_sem.at[2], a2a_sem.at[3])
    for j in (4, 5):
        permute(j).start()

    gain_load.wait()
    for copy in w_loads:
        copy.wait()

    def hidden(j, first):
        @pl.loop(0, 4)
        def _(n):
            at = pl.ds(pl.multiple_of(n * 512, 512), 512)
            part = nt(up[:, 2 * j * CW : (2 * j + 2) * CW], w[at, 2 * j * CW : (2 * j + 2) * CW])
            if first:
                gh[:, at] = part
            else:
                gh[:, at] += part

    for j in (0, 1, 2):
        permute(j).wait_recv()
        forward(j).start()
    for j in (0, 1):
        forward(j).wait_recv()
        hidden(j, j == 0)

    arrived(state, a2a_sem.at[3])
    sq_own[...] = jnp.zeros_like(sq_own)

    @pl.loop(0, HEADS)
    def _(h):
        st = jnp.concatenate([state[2 * h], state[2 * h + 1]], axis=0)
        new = att[:, lanes(h)] + jnp.exp(ccol[h]) * nn(q[:, lanes(h)], st)
        att[:, lanes(h)] = new
        sq_own[...] += new * new

    def to_sibling(src, dst, i):
        return pltpu.make_async_remote_copy(
            src_ref=src,
            dst_ref=dst,
            send_sem=tp_sem.at[2 * i],
            recv_sem=tp_sem.at[2 * i + 1],
            device_id=sibling,
            device_id_type=MESH,
        )

    squares = to_sibling(sq_own, sq_in, 0)
    squares.start()
    for j in range(2, CHUNKS):
        if j > 2:
            permute(j).wait_recv()
            forward(j).start()
        forward(j).wait_recv()
        hidden(j, False)
        if j == 2:
            squares.wait_recv()
            square_total = jnp.sum(sq_own[...] + sq_in[...], axis=1, keepdims=True)
            inv[...] = jnp.broadcast_to(
                1.0 / jnp.sqrt(square_total / FEATURES + EPS), (TOK, HEAD)
            )

    cr_own[...] = jnp.zeros_like(cr_own)

    @pl.loop(0, HEADS)
    def _(h):
        norm = gh[:, lanes(h)] * gain[:, lanes(h)]
        gh[:, lanes(h)] = norm
        cr_own[...] += norm * att[:, lanes(h)]

    crossed = to_sibling(cr_own, cr_in, 1)
    crossed.start()
    crossed.wait_recv()
    cross_total = jnp.sum(cr_own[...] + cr_in[...], axis=1, keepdims=True)
    inverse = inv[...]
    fac[...] = inverse * inverse * inverse * jnp.broadcast_to(cross_total / FEATURES, (TOK, HEAD))

    @pl.loop(0, HEADS)
    def _(h):
        grad = (inv[...] * gh[:, lanes(h)] - fac[...] * att[:, lanes(h)]).astype(BF)
        ga[:, lanes(h)] = grad
        passed = nn(wqt[h], grad).astype(BF)
        own_b[2 * h] = passed[:ROWS]
        own_b[2 * h + 1] = passed[ROWS:]

    exchange(own_b, got_b, a2a_sem.at[4], a2a_sem.at[5])

    def put(src, dst, h, i):
        pltpu.make_async_copy(src.at[:, lanes(h)], dst.at[0, :, lanes(h)], out_sem.at[i]).start()

    def gradients(h):
        qh, kh, vh, gah = q[:, lanes(h)], k[:, lanes(h)], v[:, lanes(h)], ga[:, lanes(h)]
        v0, v1, g0, g1 = vh[:HALF], vh[HALF:], gah[:HALF], gah[HALF:]
        d00, d10, d11 = decay_parts(h)
        m00 = (nt(g0, v0) * d00).astype(BF)
        m10 = (nt(g1, v0) * d10).astype(BF)
        m11 = (nt(g1, v1) * d11).astype(BF)
        st = jnp.concatenate([state[2 * h], state[2 * h + 1]], axis=0)
        head = jnp.exp(ccol[h])
        dq0 = nn(m00, kh[:HALF])
        dq1 = nn(jnp.concatenate([m10, m11], axis=1), kh)
        inter = head * nt(gah, st)
        dqs[:HALF, lanes(h)] = (dq0 + inter[:HALF]).astype(BF)
        dqs[HALF:, lanes(h)] = (dq1 + inter[HALF:]).astype(BF)
        put(dqs, dq_hbm, h, 0)
        t00, t01, t11 = turned_parts(h)
        n0 = jnp.concatenate(
            [(nt(v0, g0) * t00).astype(BF), (nt(v0, g1) * t01).astype(BF)], axis=1
        )
        n1 = (nt(v1, g1) * t11).astype(BF)
        att[:HALF, lanes(h)] = nn(n0, qh)
        att[HALF:, lanes(h)] = nn(n1, qh[HALF:])
        gh[:HALF, lanes(h)] = nn(mta[h], gah)
        gh[HALF:, lanes(h)] = nn(mtb[h], g1)

    pl.loop(0, HEADS // 2)(gradients)

    arrived(got_b, a2a_sem.at[5])
    running = jnp.zeros((ROWS, HEAD), F32)
    for b in reversed(range(BLOCKS)):
        scan_b[b] = running.astype(BF)
        running = jnp.exp(tot_in[b]) * running + got_b[b].astype(F32)
    exchange(scan_b, later, a2a_sem.at[6], a2a_sem.at[7])

    pl.loop(HEADS // 2, HEADS)(gradients)

    arrived(later, a2a_sem.at[7])

    @pl.loop(0, HEADS)
    def _(h):
        lt = jnp.concatenate([later[2 * h], later[2 * h + 1]], axis=0)
        tail = jnp.exp(totals[2 * h] - ccol[h])
        dks[:, lanes(h)] = (att[:, lanes(h)] + tail * nt(v[:, lanes(h)], lt)).astype(BF)
        put(dks, dk_hbm, h, 1)
        dvs[:, lanes(h)] = (gh[:, lanes(h)] + tail * nn(k[:, lanes(h)], lt)).astype(BF)
        put(dvs, dv_hbm, h, 2)

    for i, (src, dst) in enumerate(((dqs, dq_hbm), (dks, dk_hbm), (dvs, dv_hbm))):
        pltpu.make_async_copy(src, dst.at[0], out_sem.at[i]).wait()
    arrived(totals, tot_sem.at[0])
    for i, ref in enumerate((own_f, scan_f, own_b, scan_b)):
        arrived(ref, a2a_sem.at[2 * i])
    for j in range(CHUNKS):
        permute(j).wait_send()
        forward(j).wait_send()
    squares.wait_send()
    crossed.wait_send()


def local(queries, keys, values, upstream, out_weight, gain, log_decay):
    piece = pltpu.VMEM((BLOCKS, ROWS, HEAD), BF)
    column = pltpu.VMEM((TOK, HEAD), F32)
    rows_bf = pltpu.VMEM((TOK, WIDTH), BF)
    rows_f32 = pltpu.VMEM((TOK, WIDTH), F32)
    dma = pltpu.SemaphoreType.DMA
    hbm = pl.BlockSpec(memory_space=pl.ANY)
    out = jax.ShapeDtypeStruct((1, TOK, WIDTH), BF)
    return pl.pallas_call(
        kernel,
        out_shape=(out, out, out),
        in_specs=[hbm] * 7,
        out_specs=[hbm] * 3,
        scratch_shapes=[
            rows_bf, rows_bf, rows_bf,
            pltpu.VMEM((WIDTH, MODEL), BF),
            pltpu.VMEM((TOK, MODEL), BF),
            rows_f32, rows_f32, rows_bf,
            pltpu.VMEM((HEADS, HEAD, TOK), BF),
            pltpu.VMEM((HEADS, TOK, HEAD), F32),
            pltpu.VMEM((HEADS, TOK), F32),
            pltpu.VMEM((HEADS, HALF, TOK), BF),
            pltpu.VMEM((HEADS, HALF, HALF), BF),
            piece, piece, piece, piece, piece, piece, piece, piece,
            pltpu.VMEM((BLOCKS, 1, HEAD), F32),
            pltpu.VMEM((BLOCKS, 1, HEAD), F32),
            column, column, column, column, column, column,
            pltpu.VMEM((1, WIDTH), F32),
            pltpu.VMEM((HEADS, TOK), F32),
            rows_bf, rows_bf, rows_bf,
            dma((5 + 2 * CHUNKS,)),
            dma((2,)),
            dma((8,)),
            dma((CHUNKS,)), dma((CHUNKS,)), dma((CHUNKS,)), dma((CHUNKS,)),
            dma((4,)),
            dma((3,)),
        ],
        compiler_params=pltpu.CompilerParams(
            collective_id=0, has_side_effects=True, vmem_limit_bytes=67043328
        ),
        name="decayed_backward",
    )(queries, keys, values, upstream, out_weight, gain, log_decay)


def solution(mesh):
    torus = Mesh(
        mesh.devices.reshape(4, 4, 2, mesh.shape["tp"], mesh.shape["pp"]),
        ("seq_0", "seq_1", "seq_2", "tp", "pp"),
    )
    rows = P("pp", SEQ, "tp")
    placed = (rows, rows, rows, rows, P("pp", "tp", None), P("pp", "tp"), P("pp", "tp", SEQ))
    return jax.shard_map(
        local, mesh=torus, in_specs=placed, out_specs=(rows, rows, rows), check_vma=False
    )
```

```python
import jax
import jax.numpy as jnp
from jax import lax
from jax.experimental import pallas as pl
from jax.experimental.pallas import tpu as pltpu
from jax.sharding import Mesh
from jax.sharding import PartitionSpec as P

HEAD = 128
SEQ = ("seq_0", "seq_1", "seq_2")
MESH = pl.DeviceIdType.MESH
EPS = 1e-06
BF = jnp.bfloat16
F32 = jnp.float32

TOK = 512
HALF = 256
WIDTH = 2048
HEADS = 16
MODEL = 3072
CHUNKS = 12
CW = 128
BLOCKS = 32
ROWS = 64
FEATURES = 4096


def mark(name):
    pass


def nn(a, b):
    return lax.dot_general(a, b, (((1,), (0,)), ((), ())), preferred_element_type=F32)


def nt(a, b):
    return lax.dot_general(a, b, (((1,), (1,)), ((), ())), preferred_element_type=F32)


def lanes(h):
    return pl.ds(pl.multiple_of(h * HEAD, HEAD), HEAD)


def place(c, part):
    if c < CHUNKS - 2:
        return c // 2 * 4 * CW + part * 2 * CW + c % 2 * CW
    return (2 * c + part) * CW


def kernel(
    q_hbm, k_hbm, v_hbm, up_hbm, w_hbm, gain_hbm, ld_hbm,
    dqs, att, gh, k, v, later, ccol, totals,
    q, w, up, ga, wqt, crow, mta, mtb,
    own_f, got_f, scan_f, state, own_b, got_b, scan_b,
    tot_in, sq_own, sq_in, cr_own, cr_in, inv, fac, gain, ld,
    load_sem, tot_sem, a2a_sem, perm_send, perm_recv, fwd_send, fwd_recv, tp_sem,
):
    z, y, x = (lax.axis_index(a) for a in SEQ)
    me = z * 8 + y * 2 + x
    tp = lax.axis_index("tp")
    sibling = {"tp": 1 - tp}
    across = {"pp": 1 - lax.axis_index("pp")}

    def device_of(p):
        return {"seq_0": p // 8, "seq_1": lax.rem(p // 2, 4), "seq_2": lax.rem(p, 2)}

    def peer(i):
        p = lax.rem(me + i, BLOCKS)
        return p, device_of(p)

    mark("loads")
    loads = []

    def load(src, dst):
        copy = pltpu.make_async_copy(src, dst, load_sem.at[len(loads)])
        copy.start()
        loads.append(copy)
        return copy

    ld_load = load(ld_hbm.at[0], ld)
    k_load = load(k_hbm.at[0], k)
    v_load = load(v_hbm.at[0], v)
    q_load = load(q_hbm.at[0], q)
    gain_load = load(gain_hbm, gain)
    w_loads = []
    for j in (0, 2, 4, 6, 8, 10, 11):
        wide = CW if j >= CHUNKS - 2 else 2 * CW
        for part, side in enumerate((tp, 1 - tp)):
            at = pl.multiple_of(side * (MODEL // 2) + j * CW, CW)
            w_loads.append(
                load(w_hbm.at[0, :, pl.ds(at, wide)], w.at[:, pl.ds(place(j, part), wide)])
            )

    mark("barrier")
    barrier = pltpu.get_barrier_semaphore()

    @pl.loop(1, BLOCKS)
    def _(i):
        _, device = peer(i)
        pl.semaphore_signal(barrier, inc=1, device_id=device, device_id_type=MESH)

    pl.semaphore_signal(barrier, inc=1, device_id=sibling, device_id_type=MESH)
    pl.semaphore_signal(barrier, inc=1, device_id=across, device_id_type=MESH)
    pl.semaphore_wait(barrier, BLOCKS + 1)

    def permute(j):
        return pltpu.make_async_remote_copy(
            src_ref=up_hbm.at[0, :, pl.ds(j * CW, CW)],
            dst_ref=up.at[:, pl.ds(place(j, 0), CW)],
            send_sem=perm_send.at[j],
            recv_sem=perm_recv.at[j],
            device_id=across,
            device_id_type=MESH,
        )

    def forward(j):
        return pltpu.make_async_remote_copy(
            src_ref=up.at[:, pl.ds(place(j, 0), CW)],
            dst_ref=up.at[:, pl.ds(place(j, 1), CW)],
            send_sem=fwd_send.at[j],
            recv_sem=fwd_recv.at[j],
            device_id=sibling,
            device_id_type=MESH,
        )

    def exchange(src, dst, send_sem, recv_sem):
        @pl.loop(1, BLOCKS)
        def _(i):
            p, device = peer(i)
            pltpu.make_async_remote_copy(
                src_ref=src.at[p],
                dst_ref=dst.at[me],
                send_sem=send_sem,
                recv_sem=recv_sem,
                device_id=device,
                device_id_type=MESH,
            ).start()

        dst[me] = src[me]

    def arrived(ref, sem):
        whole = ref.at[pl.ds(0, BLOCKS - 1)]
        pltpu.make_async_copy(whole, whole, sem).wait()

    mark("perm01")
    for j in (0, 1, 2):
        permute(j).start()

    ld_load.wait()
    mark("cumsum")
    cum = ld[...]
    column_of = lax.broadcasted_iota(jnp.int32, (HEADS, TOK), 1)
    step = 1
    while step < TOK:
        moved = pltpu.roll(cum, step, 1)
        cum = cum + jnp.where(column_of >= step, moved, 0.0)
        step *= 2
    crow[...] = cum
    total = jnp.broadcast_to(cum[:, TOK - 1 : TOK], (HEADS, HEAD))
    for h in range(HEADS):
        totals[2 * h : 2 * h + 1, 0] = total[h : h + 1]
        totals[2 * h + 1 : 2 * h + 2, 0] = total[h : h + 1]
    mark("ccol")
    turned = cum.T
    for h in range(HEADS):
        ccol[h] = jnp.broadcast_to(turned[:, h : h + 1], (TOK, HEAD))

    mark("kvwait")
    k_load.wait()
    v_load.wait()

    mark("localstate")
    @pl.loop(0, HEADS, unroll=4)
    def _(h):
        tail = jnp.exp(totals[2 * h] - ccol[h])
        weighted = (k[:, lanes(h)].astype(F32) * tail).astype(BF)
        local_state = nn(weighted.T, v[:, lanes(h)]).astype(BF)
        own_f[2 * h] = local_state[:ROWS]
        own_f[2 * h + 1] = local_state[ROWS:]

    mark("a2a_f1_send")
    exchange(own_f, got_f, a2a_sem.at[0], a2a_sem.at[1])
    exchange(totals, tot_in, tot_sem.at[0], tot_sem.at[1])
    for j in (3, 4, 5):
        permute(j).start()
    q_load.wait()

    mark("intra")
    lower = lax.broadcasted_iota(jnp.int32, (HALF, HALF), 0) >= lax.broadcasted_iota(
        jnp.int32, (HALF, HALF), 1
    )
    upper = lax.broadcasted_iota(jnp.int32, (HALF, HALF), 0) <= lax.broadcasted_iota(
        jnp.int32, (HALF, HALF), 1
    )
    low = -1e30

    def decay_parts(h):
        col = ccol[h]
        col2 = jnp.concatenate([col, col], axis=1)
        row = crow[pl.ds(h, 1), :]
        c0, c1 = col2[:HALF], col2[HALF:]
        r0, r1 = row[:, :HALF], row[:, HALF:]
        d00 = jnp.exp(jnp.where(lower, c0 - r0, low))
        d10 = jnp.exp(c1 - r0)
        d11 = jnp.exp(jnp.where(lower, c1 - r1, low))
        return d00, d10, d11

    def turned_parts(h):
        col = ccol[h]
        col2 = jnp.concatenate([col, col], axis=1)
        row = crow[pl.ds(h, 1), :]
        c0, c1 = col2[:HALF], col2[HALF:]
        r0, r1 = row[:, :HALF], row[:, HALF:]
        t00 = jnp.exp(jnp.where(upper, r0 - c0, low))
        t01 = jnp.exp(r1 - c0)
        t11 = jnp.exp(jnp.where(upper, r1 - c1, low))
        return t00, t01, t11

    @pl.loop(0, HEADS)
    def _(h):
        qh, kh, vh = q[:, lanes(h)], k[:, lanes(h)], v[:, lanes(h)]
        q0, q1, k0, k1 = qh[:HALF], qh[HALF:], kh[:HALF], kh[HALF:]
        d00, d10, d11 = decay_parts(h)
        m00 = (nt(q0, k0) * d00).astype(BF)
        m10 = (nt(q1, k0) * d10).astype(BF)
        m11 = (nt(q1, k1) * d11).astype(BF)
        att[:HALF, lanes(h)] = nn(m00, vh[:HALF])
        att[HALF:, lanes(h)] = nn(jnp.concatenate([m10, m11], axis=1), vh)
        t00, t01, t11 = turned_parts(h)
        mta[h, :, :HALF] = (nt(k0, q0) * t00).astype(BF)
        mta[h, :, HALF:] = (nt(k0, q1) * t01).astype(BF)
        mtb[h] = (nt(k1, q1) * t11).astype(BF)
        wq = (qh.astype(F32) * jnp.exp(ccol[h])).astype(BF)
        wqt[h] = wq.T

    mark("wait_f1")
    arrived(tot_in, tot_sem.at[1])
    arrived(got_f, a2a_sem.at[1])
    mark("scan_f")
    running = jnp.zeros((ROWS, HEAD), F32)
    for b in range(BLOCKS):
        scan_f[b] = running.astype(BF)
        running = jnp.exp(tot_in[b]) * running + got_f[b].astype(F32)
    mark("a2a_f2_send")
    exchange(scan_f, state, a2a_sem.at[2], a2a_sem.at[3])
    for j in range(6, CHUNKS):
        permute(j).start()

    mark("wload")
    gain_load.wait()
    for copy in w_loads:
        copy.wait()

    def hidden(start, depth, first):
        @pl.loop(0, 4)
        def _(n):
            at = pl.ds(pl.multiple_of(n * 512, 512), 512)
            part = nt(up[:, start : start + depth], w[at, start : start + depth])
            if first:
                gh[:, at] = part
            else:
                gh[:, at] += part

    def relay(*chunks):
        for j in chunks:
            permute(j).wait_recv()
            forward(j).start()

    def relayed(*chunks):
        for j in chunks:
            forward(j).wait_recv()

    mark("relay012")
    relay(0, 1, 2, 3)
    relayed(0, 1)
    mark("hidden01")
    hidden(0, 512, True)
    mark("relay4")
    relay(4)
    relayed(2, 3)
    mark("hidden23")
    hidden(512, 512, False)
    mark("relay5")
    relay(5)
    relayed(4, 5)
    mark("hidden45")
    hidden(1024, 512, False)

    mark("wait_f2")
    arrived(state, a2a_sem.at[3])
    mark("att_inter")
    sq_own[...] = jnp.zeros_like(sq_own)

    @pl.loop(0, HEADS, unroll=4)
    def _(h):
        st = jnp.concatenate([state[2 * h], state[2 * h + 1]], axis=0)
        new = att[:, lanes(h)] + jnp.exp(ccol[h]) * nn(q[:, lanes(h)], st)
        att[:, lanes(h)] = new
        sq_own[...] += new * new

    def to_sibling(src, dst, i):
        return pltpu.make_async_remote_copy(
            src_ref=src,
            dst_ref=dst,
            send_sem=tp_sem.at[2 * i],
            recv_sem=tp_sem.at[2 * i + 1],
            device_id=sibling,
            device_id_type=MESH,
        )

    squares = to_sibling(sq_own, sq_in, 0)
    squares.start()
    mark("relay67")
    relay(6, 7)
    squares.wait_recv()
    mark("inverse")
    square_total = jnp.sum(sq_own[...] + sq_in[...], axis=1, keepdims=True)
    inv[...] = jnp.broadcast_to(1.0 / jnp.sqrt(square_total / FEATURES + EPS), (TOK, HEAD))
    relayed(6, 7)
    mark("hidden67")
    hidden(1536, 512, False)
    mark("relay89")
    relay(8, 9)
    relayed(8, 9)
    mark("hidden89")
    hidden(2048, 512, False)
    mark("relay10")
    relay(10)
    relayed(10)
    mark("hidden10")
    hidden(2560, 256, False)
    mark("relay11")
    relay(11)
    cr_own[...] = jnp.zeros_like(cr_own)
    relayed(11)
    mark("hidden11")

    @pl.loop(0, 4)
    def _(n):
        at = pl.ds(pl.multiple_of(n * 512, 512), 512)
        norm = (gh[:, at] + nt(up[:, 2816:], w[at, 2816:])) * gain[:, at]
        gh[:, at] = norm
        both = norm * att[:, at]
        cr_own[...] += (both[:, :128] + both[:, 128:256]) + (both[:, 256:384] + both[:, 384:])

    crossed = to_sibling(cr_own, cr_in, 1)
    crossed.start()
    mark("cross_wait")
    crossed.wait_recv()
    cross_total = jnp.sum(cr_own[...] + cr_in[...], axis=1, keepdims=True)
    inverse = inv[...]
    fac[...] = inverse * inverse * inverse * jnp.broadcast_to(cross_total / FEATURES, (TOK, HEAD))

    mark("ga_passed")
    @pl.loop(0, HEADS, unroll=2)
    def _(i):
        h = lax.rem(me // 2 + i, HEADS)
        grad = (inv[...] * gh[:, lanes(h)] - fac[...] * att[:, lanes(h)]).astype(BF)
        ga[:, lanes(h)] = grad
        passed = nn(wqt[h], grad).astype(BF)
        own_b[2 * h] = passed[:ROWS]
        own_b[2 * h + 1] = passed[ROWS:]
        for side in (0, 1):
            p = 2 * h + side

            @pl.when(p != me)
            def _():
                pltpu.make_async_remote_copy(
                    src_ref=own_b.at[p],
                    dst_ref=got_b.at[me],
                    send_sem=a2a_sem.at[4],
                    recv_sem=a2a_sem.at[5],
                    device_id=device_of(p),
                    device_id_type=MESH,
                ).start()

    got_b[me] = own_b[me]

    def gradients(h):
        qh, kh, vh, gah = q[:, lanes(h)], k[:, lanes(h)], v[:, lanes(h)], ga[:, lanes(h)]
        v0, v1, g0, g1 = vh[:HALF], vh[HALF:], gah[:HALF], gah[HALF:]
        d00, d10, d11 = decay_parts(h)
        m00 = (nt(g0, v0) * d00).astype(BF)
        m10 = (nt(g1, v0) * d10).astype(BF)
        m11 = (nt(g1, v1) * d11).astype(BF)
        st = jnp.concatenate([state[2 * h], state[2 * h + 1]], axis=0)
        head = jnp.exp(ccol[h])
        dq0 = nn(m00, kh[:HALF])
        dq1 = nn(jnp.concatenate([m10, m11], axis=1), kh)
        inter = head * nt(gah, st)
        dqs[:HALF, lanes(h)] = (dq0 + inter[:HALF]).astype(BF)
        dqs[HALF:, lanes(h)] = (dq1 + inter[HALF:]).astype(BF)
        t00, t01, t11 = turned_parts(h)
        n0 = jnp.concatenate(
            [(nt(v0, g0) * t00).astype(BF), (nt(v0, g1) * t01).astype(BF)], axis=1
        )
        n1 = (nt(v1, g1) * t11).astype(BF)
        att[:HALF, lanes(h)] = nn(n0, qh)
        att[HALF:, lanes(h)] = nn(n1, qh[HALF:])
        gh[:HALF, lanes(h)] = nn(mta[h], gah)
        gh[HALF:, lanes(h)] = nn(mtb[h], g1)

    mark("grad1")
    pl.loop(0, HEADS // 2)(gradients)

    mark("wait_b1")
    arrived(got_b, a2a_sem.at[5])
    mark("scan_b")
    running = jnp.zeros((ROWS, HEAD), F32)
    for b in reversed(range(BLOCKS)):
        scan_b[b] = running.astype(BF)
        running = jnp.exp(tot_in[b]) * running + got_b[b].astype(F32)
    mark("a2a_b2_send")
    exchange(scan_b, later, a2a_sem.at[6], a2a_sem.at[7])

    mark("grad2")
    pl.loop(HEADS // 2, HEADS)(gradients)

    mark("wait_b2")
    arrived(later, a2a_sem.at[7])

    mark("sendwaits")
    arrived(totals, tot_sem.at[0])
    for i, ref in enumerate((own_f, scan_f, own_b, scan_b)):
        arrived(ref, a2a_sem.at[2 * i])
    for j in range(CHUNKS):
        permute(j).wait_send()
        forward(j).wait_send()
    squares.wait_send()
    crossed.wait_send()
    mark(None)


def finish(
    dqs, att, gh, k, v, later, ccol, totals, dq_hbm, dk_hbm, dv_hbm, dks, dvs, out_sem
):
    pltpu.make_async_copy(dqs, dq_hbm.at[0], out_sem.at[0]).start()

    def put(src, dst, h, i):
        pltpu.make_async_copy(src.at[:, lanes(h)], dst.at[0, :, lanes(h)], out_sem.at[i]).start()

    @pl.loop(0, HEADS, unroll=2)
    def _(h):
        lt = jnp.concatenate([later[2 * h], later[2 * h + 1]], axis=0)
        tail = jnp.exp(totals[2 * h] - ccol[h])
        dks[:, lanes(h)] = (att[:, lanes(h)] + tail * nt(v[:, lanes(h)], lt)).astype(BF)
        put(dks, dk_hbm, h, 1)
        dvs[:, lanes(h)] = (gh[:, lanes(h)] + tail * nn(k[:, lanes(h)], lt)).astype(BF)
        put(dvs, dv_hbm, h, 2)

    for i, (src, dst) in enumerate(((dqs, dq_hbm), (dks, dk_hbm), (dvs, dv_hbm))):
        pltpu.make_async_copy(src, dst.at[0], out_sem.at[i]).wait()


def local(queries, keys, values, upstream, out_weight, gain, log_decay):
    vmem = pltpu.VMEM
    piece = vmem((BLOCKS, ROWS, HEAD), BF)
    column = vmem((TOK, HEAD), F32)
    rows_bf = vmem((TOK, WIDTH), BF)
    rows_f32 = vmem((TOK, WIDTH), F32)
    columns = vmem((HEADS, TOK, HEAD), F32)
    totals = vmem((BLOCKS, 1, HEAD), F32)
    dma = pltpu.SemaphoreType.DMA
    hbm = pl.BlockSpec(memory_space=pl.ANY)
    here = pl.BlockSpec(memory_space=vmem)
    kept = pl.pallas_call(
        kernel,
        out_shape=(rows_bf, rows_f32, rows_f32, rows_bf, rows_bf, piece, columns, totals),
        in_specs=[hbm] * 7,
        out_specs=[here] * 8,
        scratch_shapes=[
            rows_bf,
            vmem((WIDTH, MODEL), BF),
            vmem((TOK, MODEL), BF),
            rows_bf,
            vmem((HEADS, HEAD, TOK), BF),
            vmem((HEADS, TOK), F32),
            vmem((HEADS, HALF, TOK), BF),
            vmem((HEADS, HALF, HALF), BF),
            piece, piece, piece, piece, piece, piece, piece,
            totals,
            column, column, column, column, column, column,
            vmem((1, WIDTH), F32),
            vmem((HEADS, TOK), F32),
            dma((19,)),
            dma((2,)),
            dma((8,)),
            dma((CHUNKS,)), dma((CHUNKS,)), dma((CHUNKS,)), dma((CHUNKS,)),
            dma((4,)),
        ],
        compiler_params=pltpu.CompilerParams(
            collective_id=0, has_side_effects=True, vmem_limit_bytes=45 << 20
        ),
        name="decayed_backward",
    )(queries, keys, values, upstream, out_weight, gain, log_decay)
    out = jax.ShapeDtypeStruct((1, TOK, WIDTH), BF)
    return pl.pallas_call(
        finish,
        out_shape=(out, out, out),
        in_specs=[here] * 8,
        out_specs=[hbm] * 3,
        scratch_shapes=[rows_bf, rows_bf, dma((3,))],
        compiler_params=pltpu.CompilerParams(vmem_limit_bytes=24 << 20),
        name="finish",
    )(*kept)


def solution(mesh):
    torus = Mesh(
        mesh.devices.reshape(4, 4, 2, mesh.shape["tp"], mesh.shape["pp"]),
        ("seq_0", "seq_1", "seq_2", "tp", "pp"),
    )
    rows = P("pp", SEQ, "tp")
    placed = (rows, rows, rows, rows, P("pp", "tp", None), P("pp", "tp"), P("pp", "tp", SEQ))
    return jax.shard_map(
        local, mesh=torus, in_specs=placed, out_specs=(rows, rows, rows), check_vma=False
    )
```

```python
import jax
import jax.numpy as jnp
from jax import lax
from jax.experimental import pallas as pl
from jax.experimental.pallas import tpu as pltpu
from jax.sharding import Mesh
from jax.sharding import PartitionSpec as P

HEAD = 128
SEQ = ("seq_0", "seq_1", "seq_2")
MESH = pl.DeviceIdType.MESH
EPS = 1e-06
BF = jnp.bfloat16
F32 = jnp.float32

TOK = 512
HALF = 256
WIDTH = 2048
HEADS = 16
MODEL = 3072
CHUNKS = 12
CW = 128
BLOCKS = 32
ROWS = 64
FEATURES = 4096


def mark(name):
    pass


def nn(a, b):
    return lax.dot_general(a, b, (((1,), (0,)), ((), ())), preferred_element_type=F32)


def nt(a, b):
    return lax.dot_general(a, b, (((1,), (1,)), ((), ())), preferred_element_type=F32)


def lanes(h):
    return pl.ds(pl.multiple_of(h * HEAD, HEAD), HEAD)


def pair_lanes(i):
    return pl.ds(pl.multiple_of(i * 2 * HEAD, 2 * HEAD), 2 * HEAD)


def two_states(ref, i):
    none = jnp.zeros((HEAD, HEAD), BF)
    first = jnp.concatenate([ref[4 * i], ref[4 * i + 1]], axis=0)
    second = jnp.concatenate([ref[4 * i + 2], ref[4 * i + 3]], axis=0)
    return jnp.concatenate(
        [jnp.concatenate([first, none], axis=1), jnp.concatenate([none, second], axis=1)], axis=0
    )


def two_columns(ref, i):
    return jnp.concatenate([ref[2 * i], ref[2 * i + 1]], axis=1)


def place(c, part):
    if c < CHUNKS - 2:
        return c // 2 * 4 * CW + part * 2 * CW + c % 2 * CW
    return (2 * c + part) * CW


def kernel(
    q_hbm, k_hbm, v_hbm, up_hbm, w_hbm, gain_hbm, ld_hbm,
    dqs, att, gh, k, v, later, ccol, totals,
    q, w, up, ga, wqt, crow, mta, mtb,
    own_f, got_f, scan_f, state, own_b, got_b, scan_b,
    tot_in, sq_own, sq_in, cr_own, cr_in, inv, fac, gain, ld, b_own, b_in,
    load_sem, tot_sem, a2a_sem, perm_send, perm_recv, fwd_send, fwd_recv, tp_sem, b_sem,
):
    z, y, x = (lax.axis_index(a) for a in SEQ)
    me = z * 8 + y * 2 + x
    tp = lax.axis_index("tp")
    sibling = {"tp": 1 - tp}
    across = {"pp": 1 - lax.axis_index("pp")}

    def device_of(p):
        return {"seq_0": p // 8, "seq_1": lax.rem(p // 2, 4), "seq_2": lax.rem(p, 2)}

    zs = [lax.rem(z + d, 4) for d in range(4)]
    ys = [lax.rem(y + d, 4) for d in range(4)]
    xs = [x, 1 - x]
    peers = [
        (zs[i] * 8 + ys[j] * 2 + xs[k], {"seq_0": zs[i], "seq_1": ys[j], "seq_2": xs[k]})
        for i in range(4)
        for j in range(4)
        for k in range(2)
    ][1:]

    mark("loads")
    loads = []

    def load(src, dst):
        copy = pltpu.make_async_copy(src, dst, load_sem.at[len(loads)])
        copy.start()
        loads.append(copy)
        return copy

    ld_load = load(ld_hbm.at[0], ld)
    k_load = load(k_hbm.at[0], k)
    v_load = load(v_hbm.at[0], v)
    q_load = load(q_hbm.at[0], q)
    gain_load = load(gain_hbm, gain)
    w_loads = []
    for j in (0, 2, 4, 6, 8, 10, 11):
        wide = CW if j >= CHUNKS - 2 else 2 * CW
        for part, side in enumerate((tp, 1 - tp)):
            at = pl.multiple_of(side * (MODEL // 2) + j * CW, CW)
            w_loads.append(
                load(w_hbm.at[0, :, pl.ds(at, wide)], w.at[:, pl.ds(place(j, part), wide)])
            )

    mark("barrier")
    barrier = pltpu.get_barrier_semaphore()

    for _, device in peers:
        pl.semaphore_signal(barrier, inc=1, device_id=device, device_id_type=MESH)
    pl.semaphore_signal(barrier, inc=1, device_id=sibling, device_id_type=MESH)
    pl.semaphore_signal(barrier, inc=1, device_id=across, device_id_type=MESH)
    pl.semaphore_wait(barrier, BLOCKS + 1)

    def permute(j):
        return pltpu.make_async_remote_copy(
            src_ref=up_hbm.at[0, :, pl.ds(j * CW, CW)],
            dst_ref=up.at[:, pl.ds(place(j, 0), CW)],
            send_sem=perm_send.at[j],
            recv_sem=perm_recv.at[j],
            device_id=across,
            device_id_type=MESH,
        )

    def forward(j):
        return pltpu.make_async_remote_copy(
            src_ref=up.at[:, pl.ds(place(j, 0), CW)],
            dst_ref=up.at[:, pl.ds(place(j, 1), CW)],
            send_sem=fwd_send.at[j],
            recv_sem=fwd_recv.at[j],
            device_id=sibling,
            device_id_type=MESH,
        )

    def exchange(src, dst, send_sem, recv_sem):
        for p, device in peers:
            pltpu.make_async_remote_copy(
                src_ref=src.at[p],
                dst_ref=dst.at[me],
                send_sem=send_sem,
                recv_sem=recv_sem,
                device_id=device,
                device_id_type=MESH,
            ).start()
        dst[me] = src[me]

    def arrived(ref, sem):
        whole = ref.at[pl.ds(0, BLOCKS - 1)]
        pltpu.make_async_copy(whole, whole, sem).wait()

    mark("perm01")
    for j in (0, 1):
        permute(j).start()

    ld_load.wait()
    mark("cumsum")
    cum = ld[...]
    column_of = lax.broadcasted_iota(jnp.int32, (HEADS, TOK), 1)
    step = 1
    while step < TOK:
        moved = pltpu.roll(cum, step, 1)
        cum = cum + jnp.where(column_of >= step, moved, 0.0)
        step *= 2
    crow[...] = cum
    total = jnp.broadcast_to(cum[:, TOK - 1 : TOK], (HEADS, HEAD))
    for h in range(HEADS):
        totals[2 * h : 2 * h + 1, 0] = total[h : h + 1]
        totals[2 * h + 1 : 2 * h + 2, 0] = total[h : h + 1]
    mark("ccol")
    turned = cum.T
    for h in range(HEADS):
        ccol[h] = jnp.broadcast_to(turned[:, h : h + 1], (TOK, HEAD))

    mark("kvwait")
    k_load.wait()
    v_load.wait()

    mark("localstate")
    @pl.loop(0, HEADS, unroll=4)
    def _(h):
        tail = jnp.exp(totals[2 * h] - ccol[h])
        weighted = (k[:, lanes(h)].astype(F32) * tail).astype(BF)
        local_state = nn(weighted.T, v[:, lanes(h)]).astype(BF)
        own_f[2 * h] = local_state[:ROWS]
        own_f[2 * h + 1] = local_state[ROWS:]

    mark("a2a_f1_send")
    exchange(own_f, got_f, a2a_sem.at[0], a2a_sem.at[1])
    exchange(totals, tot_in, tot_sem.at[0], tot_sem.at[1])
    for j in (2, 3, 4):
        permute(j).start()
    q_load.wait()

    mark("intra")
    lower = lax.broadcasted_iota(jnp.int32, (HALF, HALF), 0) >= lax.broadcasted_iota(
        jnp.int32, (HALF, HALF), 1
    )
    upper = lax.broadcasted_iota(jnp.int32, (HALF, HALF), 0) <= lax.broadcasted_iota(
        jnp.int32, (HALF, HALF), 1
    )
    low = -1e30

    def decay_parts(h):
        col = ccol[h]
        col2 = jnp.concatenate([col, col], axis=1)
        row = crow[pl.ds(h, 1), :]
        c0, c1 = col2[:HALF], col2[HALF:]
        r0, r1 = row[:, :HALF], row[:, HALF:]
        d00 = jnp.exp(jnp.where(lower, c0 - r0, low))
        d10 = jnp.exp(c1 - r0)
        d11 = jnp.exp(jnp.where(lower, c1 - r1, low))
        return d00, d10, d11

    def turned_parts(h):
        col = ccol[h]
        col2 = jnp.concatenate([col, col], axis=1)
        row = crow[pl.ds(h, 1), :]
        c0, c1 = col2[:HALF], col2[HALF:]
        r0, r1 = row[:, :HALF], row[:, HALF:]
        t00 = jnp.exp(jnp.where(upper, r0 - c0, low))
        t01 = jnp.exp(r1 - c0)
        t11 = jnp.exp(jnp.where(upper, r1 - c1, low))
        return t00, t01, t11

    @pl.loop(0, HEADS)
    def _(h):
        qh, kh, vh = q[:, lanes(h)], k[:, lanes(h)], v[:, lanes(h)]
        q0, q1, k0, k1 = qh[:HALF], qh[HALF:], kh[:HALF], kh[HALF:]
        d00, d10, d11 = decay_parts(h)
        m00 = (nt(q0, k0) * d00).astype(BF)
        m10 = (nt(q1, k0) * d10).astype(BF)
        m11 = (nt(q1, k1) * d11).astype(BF)
        att[:HALF, lanes(h)] = nn(m00, vh[:HALF])
        att[HALF:, lanes(h)] = nn(jnp.concatenate([m10, m11], axis=1), vh)
        t00, t01, t11 = turned_parts(h)
        mta[h, :, :HALF] = (nt(k0, q0) * t00).astype(BF)
        mta[h, :, HALF:] = (nt(k0, q1) * t01).astype(BF)
        mtb[h] = (nt(k1, q1) * t11).astype(BF)
        wq = (qh.astype(F32) * jnp.exp(ccol[h])).astype(BF)
        wqt[h] = wq.T

    mark("wait_f1")
    arrived(tot_in, tot_sem.at[1])
    arrived(got_f, a2a_sem.at[1])
    mark("scan_f")
    running = jnp.zeros((ROWS, HEAD), F32)
    for b in range(BLOCKS):
        scan_f[b] = running.astype(BF)
        running = jnp.exp(tot_in[b]) * running + got_f[b].astype(F32)
    mark("a2a_f2_send")
    exchange(scan_f, state, a2a_sem.at[2], a2a_sem.at[3])
    for j in range(5, CHUNKS):
        permute(j).start()

    mark("wload")
    gain_load.wait()
    for copy in w_loads:
        copy.wait()

    def hidden(start, depth, first):
        @pl.loop(0, 4)
        def _(n):
            at = pl.ds(pl.multiple_of(n * 512, 512), 512)
            part = nt(up[:, start : start + depth], w[at, start : start + depth])
            if first:
                gh[:, at] = part
            else:
                gh[:, at] += part

    def relay(*chunks):
        for j in chunks:
            permute(j).wait_recv()
            forward(j).start()

    def relayed(*chunks):
        for j in chunks:
            forward(j).wait_recv()

    mark("relay012")
    relay(0, 1, 2, 3)
    relayed(0, 1)
    mark("hidden01")
    hidden(0, 512, True)
    mark("relay23")
    relay(4)
    relayed(2, 3)
    mark("hidden23")
    hidden(512, 512, False)

    mark("wait_f2")
    arrived(state, a2a_sem.at[3])
    mark("att_inter")
    sq_own[...] = jnp.zeros_like(sq_own)

    @pl.loop(0, HEADS // 2, unroll=2)
    def _(i):
        at = pair_lanes(i)
        new = att[:, at] + jnp.exp(two_columns(ccol, i)) * nn(q[:, at], two_states(state, i))
        att[:, at] = new
        ga[:, at] = (new * gain[:, at]).astype(BF)
        both = new * new
        sq_own[...] += both[:, :HEAD] + both[:, HEAD:]

    def to_sibling(src, dst, i):
        return pltpu.make_async_remote_copy(
            src_ref=src,
            dst_ref=dst,
            send_sem=tp_sem.at[2 * i],
            recv_sem=tp_sem.at[2 * i + 1],
            device_id=sibling,
            device_id_type=MESH,
        )

    def tail_product():
        b_own[...] = nn(ga[...], w[:, 2560:]).astype(BF)
        for at in range(0, 4 * CW, CW):
            copy = pltpu.make_async_remote_copy(
                src_ref=b_own.at[:, pl.ds(at, CW)],
                dst_ref=b_in.at[:, pl.ds(at + CW if at % (2 * CW) == 0 else at - CW, CW)],
                send_sem=b_sem.at[0],
                recv_sem=b_sem.at[1],
                device_id=sibling,
                device_id_type=MESH,
            )
            copy.start()

    squares = to_sibling(sq_own, sq_in, 0)
    squares.start()
    cr_own[...] = jnp.zeros_like(cr_own)
    mark("tail_product")
    tail_product()
    mark("relay45")
    relay(5)
    relayed(4, 5)
    mark("hidden45")
    hidden(1024, 512, False)
    mark("inverse")
    squares.wait_recv()
    square_total = jnp.sum(sq_own[...] + sq_in[...], axis=1, keepdims=True)
    inv[...] = jnp.broadcast_to(1.0 / jnp.sqrt(square_total / FEATURES + EPS), (TOK, HEAD))
    mark("relay67")
    relay(6, 7)
    relayed(6, 7)
    mark("hidden67")
    hidden(1536, 512, False)
    mark("relay89")
    relay(8, 9)
    relayed(8, 9)
    mark("hidden89")

    @pl.loop(0, 4)
    def _(n):
        at = pl.ds(pl.multiple_of(n * 512, 512), 512)
        new = gh[:, at] + nt(up[:, 2048:2560], w[at, 2048:2560])
        gh[:, at] = new
        both = new * gain[:, at] * att[:, at]
        cr_own[...] += (both[:, :128] + both[:, 128:256]) + (both[:, 256:384] + both[:, 384:])

    crossed = to_sibling(cr_own, cr_in, 1)
    crossed.start()
    mark("relay10")
    relay(10)
    mark("wait_b_in")
    pltpu.make_async_copy(b_in, b_in, b_sem.at[1]).wait()
    mark("relayed10")
    relayed(10)
    mark("hidden10")
    hidden(2560, 256, False)
    mark("relay11")
    crossed.wait_recv()
    relay(11)
    relayed(11)
    mark("crossing11")
    part = cr_own[...] + cr_in[...]
    for at in range(0, 4 * CW, CW):
        both = b_own[:, at : at + CW].astype(F32) + b_in[:, at : at + CW].astype(F32)
        part += up[:, 2560 + at : 2560 + at + CW].astype(F32) * both
    cross_total = jnp.sum(part, axis=1, keepdims=True)
    inverse = inv[...]
    fac[...] = inverse * inverse * inverse * jnp.broadcast_to(cross_total / FEATURES, (TOK, HEAD))

    mark("ga_passed")
    low_rows, high_rows = pl.ds(0, ROWS // 2), pl.ds(ROWS // 2, ROWS // 2)

    def send_piece(src, dst, p, device, rows, sem):
        pltpu.make_async_remote_copy(
            src_ref=src.at[p, rows],
            dst_ref=dst.at[me, rows],
            send_sem=a2a_sem.at[sem],
            recv_sem=a2a_sem.at[sem + 1],
            device_id=device,
            device_id_type=MESH,
        ).start()

    def piece_arrived(ref, rows, sem):
        whole = ref.at[pl.ds(0, BLOCKS - 1), rows]
        pltpu.make_async_copy(whole, whole, a2a_sem.at[sem]).wait()

    groups = [lax.rem(me // 8 + n, 4) for n in range(4)]

    def normed(n):
        at = pl.ds(pl.multiple_of(groups[n] * 512, 512), 512)
        return (gh[:, at] + nt(up[:, 2816:], w[at, 2816:])) * gain[:, at]

    norm = normed(0)
    for n in range(4):
        g = groups[n]
        after = normed(n + 1) if n < 3 else None
        for j in range(4):
            h = 4 * g + j
            grad = inv[...] * norm[:, j * HEAD : (j + 1) * HEAD] - fac[...] * att[:, lanes(h)]
            grad = grad.astype(BF)
            ga[:, lanes(h)] = grad
            passed = nn(wqt[h], grad).astype(BF)
            own_b[2 * h] = passed[:ROWS]
            own_b[2 * h + 1] = passed[ROWS:]
        for s in range(8):
            if n > 0 or s > 0:
                p = 8 * g + lax.rem(me + s, 8)
                send_piece(own_b, got_b, p, device_of(p), low_rows, 4)
        norm = after
    mark("send_high")
    for p, device in peers:
        send_piece(own_b, got_b, p, device, high_rows, 6)
    got_b[me] = own_b[me]

    def gradients(h):
        qh, kh, vh, gah = q[:, lanes(h)], k[:, lanes(h)], v[:, lanes(h)], ga[:, lanes(h)]
        v0, v1, g0, g1 = vh[:HALF], vh[HALF:], gah[:HALF], gah[HALF:]
        d00, d10, d11 = decay_parts(h)
        m00 = (nt(g0, v0) * d00).astype(BF)
        m10 = (nt(g1, v0) * d10).astype(BF)
        m11 = (nt(g1, v1) * d11).astype(BF)
        st = jnp.concatenate([state[2 * h], state[2 * h + 1]], axis=0)
        head = jnp.exp(ccol[h])
        dq0 = nn(m00, kh[:HALF])
        dq1 = nn(jnp.concatenate([m10, m11], axis=1), kh)
        inter = head * nt(gah, st)
        dqs[:HALF, lanes(h)] = (dq0 + inter[:HALF]).astype(BF)
        dqs[HALF:, lanes(h)] = (dq1 + inter[HALF:]).astype(BF)
        t00, t01, t11 = turned_parts(h)
        n0 = jnp.concatenate(
            [(nt(v0, g0) * t00).astype(BF), (nt(v0, g1) * t01).astype(BF)], axis=1
        )
        n1 = (nt(v1, g1) * t11).astype(BF)
        att[:HALF, lanes(h)] = nn(n0, qh)
        att[HALF:, lanes(h)] = nn(n1, qh[HALF:])
        gh[:HALF, lanes(h)] = nn(mta[h], gah)
        gh[HALF:, lanes(h)] = nn(mtb[h], g1)

    def scan_back(rows):
        running = jnp.zeros((ROWS // 2, HEAD), F32)
        for b in reversed(range(BLOCKS)):
            scan_b[b, rows] = running.astype(BF)
            running = jnp.exp(tot_in[b]) * running + got_b[b, rows].astype(F32)
        for p, device in peers:
            send_piece(scan_b, later, p, device, rows, 8 if rows is low_rows else 10)
        later[me, rows] = scan_b[me, rows]

    mark("grad1")
    pl.loop(0, 4)(gradients)
    mark("wait_b1a")
    piece_arrived(got_b, low_rows, 5)
    mark("scan_ba")
    scan_back(low_rows)
    mark("grad2")
    pl.loop(4, 7)(gradients)
    mark("wait_b1b")
    piece_arrived(got_b, high_rows, 7)
    mark("scan_bb")
    scan_back(high_rows)
    mark("grad3")
    pl.loop(7, HEADS)(gradients)
    mark("wait_b2")
    piece_arrived(later, low_rows, 9)
    piece_arrived(later, high_rows, 11)

    mark("sendwaits")
    arrived(totals, tot_sem.at[0])
    arrived(own_f, a2a_sem.at[0])
    arrived(scan_f, a2a_sem.at[2])
    for rows, sem in ((low_rows, 4), (high_rows, 6)):
        piece_arrived(own_b, rows, sem)
        piece_arrived(scan_b, rows, sem + 4)
    pltpu.make_async_copy(b_own, b_own, b_sem.at[0]).wait()
    for j in range(CHUNKS):
        permute(j).wait_send()
        forward(j).wait_send()
    squares.wait_send()
    crossed.wait_send()
    mark(None)


def finish(
    dqs, att, gh, k, v, later, ccol, totals, dq_hbm, dk_hbm, dv_hbm, dks, dvs, out_sem
):
    pltpu.make_async_copy(dqs, dq_hbm.at[0], out_sem.at[0]).start()

    def put(src, dst, at, i):
        pltpu.make_async_copy(src.at[:, at], dst.at[0, :, at], out_sem.at[i]).start()

    @pl.loop(0, HEADS // 2, unroll=2)
    def _(i):
        at = pair_lanes(i)
        lt = two_states(later, i)
        total = jnp.concatenate([totals[4 * i], totals[4 * i + 2]], axis=1)
        tail = jnp.exp(total - two_columns(ccol, i))
        dks[:, at] = (att[:, at] + tail * nt(v[:, at], lt)).astype(BF)
        put(dks, dk_hbm, at, 1)
        dvs[:, at] = (gh[:, at] + tail * nn(k[:, at], lt)).astype(BF)
        put(dvs, dv_hbm, at, 2)

    for i, (src, dst) in enumerate(((dqs, dq_hbm), (dks, dk_hbm), (dvs, dv_hbm))):
        pltpu.make_async_copy(src, dst.at[0], out_sem.at[i]).wait()


def local(queries, keys, values, upstream, out_weight, gain, log_decay):
    vmem = pltpu.VMEM
    piece = vmem((BLOCKS, ROWS, HEAD), BF)
    column = vmem((TOK, HEAD), F32)
    rows_bf = vmem((TOK, WIDTH), BF)
    rows_f32 = vmem((TOK, WIDTH), F32)
    columns = vmem((HEADS, TOK, HEAD), F32)
    totals = vmem((BLOCKS, 1, HEAD), F32)
    dma = pltpu.SemaphoreType.DMA
    hbm = pl.BlockSpec(memory_space=pl.ANY)
    here = pl.BlockSpec(memory_space=vmem)
    kept = pl.pallas_call(
        kernel,
        out_shape=(rows_bf, rows_f32, rows_f32, rows_bf, rows_bf, piece, columns, totals),
        in_specs=[hbm] * 7,
        out_specs=[here] * 8,
        scratch_shapes=[
            rows_bf,
            vmem((WIDTH, MODEL), BF),
            vmem((TOK, MODEL), BF),
            rows_bf,
            vmem((HEADS, HEAD, TOK), BF),
            vmem((HEADS, TOK), F32),
            vmem((HEADS, HALF, TOK), BF),
            vmem((HEADS, HALF, HALF), BF),
            piece, piece, piece, piece, piece, piece, piece,
            totals,
            column, column, column, column, column, column,
            vmem((1, WIDTH), F32),
            vmem((HEADS, TOK), F32),
            vmem((TOK, 4 * CW), BF),
            vmem((TOK, 4 * CW), BF),
            dma((19,)),
            dma((2,)),
            dma((12,)),
            dma((CHUNKS,)), dma((CHUNKS,)), dma((CHUNKS,)), dma((CHUNKS,)),
            dma((4,)),
            dma((2,)),
        ],
        compiler_params=pltpu.CompilerParams(
            collective_id=0, has_side_effects=True, vmem_limit_bytes=45 << 20
        ),
        name="decayed_backward",
    )(queries, keys, values, upstream, out_weight, gain, log_decay)
    out = jax.ShapeDtypeStruct((1, TOK, WIDTH), BF)
    return pl.pallas_call(
        finish,
        out_shape=(out, out, out),
        in_specs=[here] * 8,
        out_specs=[hbm] * 3,
        scratch_shapes=[rows_bf, rows_bf, dma((3,))],
        compiler_params=pltpu.CompilerParams(vmem_limit_bytes=24 << 20),
        name="finish",
    )(*kept)


def solution(mesh):
    torus = Mesh(
        mesh.devices.reshape(4, 4, 2, mesh.shape["tp"], mesh.shape["pp"]),
        ("seq_0", "seq_1", "seq_2", "tp", "pp"),
    )
    rows = P("pp", SEQ, "tp")
    placed = (rows, rows, rows, rows, P("pp", "tp", None), P("pp", "tp"), P("pp", "tp", SEQ))
    return jax.shard_map(
        local, mesh=torus, in_specs=placed, out_specs=(rows, rows, rows), check_vma=False
    )
```

```python
import jax
import jax.numpy as jnp
from jax import lax
from jax.experimental import pallas as pl
from jax.experimental.pallas import tpu as pltpu
from jax.sharding import Mesh
from jax.sharding import PartitionSpec as P

HEAD = 128
SEQ = ("seq_0", "seq_1", "seq_2")
MESH = pl.DeviceIdType.MESH
EPS = 1e-06
BF = jnp.bfloat16
F32 = jnp.float32

TOK = 512
HALF = 256
WIDTH = 2048
HEADS = 16
MODEL = 3072
CHUNKS = 12
CW = 128
BLOCKS = 32
ROWS = 64
FEATURES = 4096


def mark(name):
    pass


def nn(a, b):
    return lax.dot_general(a, b, (((1,), (0,)), ((), ())), preferred_element_type=F32)


def nt(a, b):
    return lax.dot_general(a, b, (((1,), (1,)), ((), ())), preferred_element_type=F32)


def lanes(h):
    return pl.ds(pl.multiple_of(h * HEAD, HEAD), HEAD)


def pair_lanes(i):
    return pl.ds(pl.multiple_of(i * 2 * HEAD, 2 * HEAD), 2 * HEAD)


def two_states(ref, i):
    none = jnp.zeros((HEAD, HEAD), BF)
    first = jnp.concatenate([ref[4 * i], ref[4 * i + 1]], axis=0)
    second = jnp.concatenate([ref[4 * i + 2], ref[4 * i + 3]], axis=0)
    return jnp.concatenate(
        [jnp.concatenate([first, none], axis=1), jnp.concatenate([none, second], axis=1)], axis=0
    )


def two_columns(ref, i):
    return jnp.concatenate([ref[2 * i], ref[2 * i + 1]], axis=1)


def place(c, part):
    if c < CHUNKS - 2:
        return c // 2 * 4 * CW + part * 2 * CW + c % 2 * CW
    return (2 * c + part) * CW


def kernel(
    q_hbm, k_hbm, v_hbm, up_hbm, w_hbm, gain_hbm, ld_hbm,
    dqs, att, gh, k, v, later, tails,
    ccol, totals, q, w, up, ga, wqt, crow, mta, mtb,
    own_f, got_f, scan_f, state, own_b, got_b, scan_b,
    tot_in, sq_own, sq_in, cr_own, cr_in, inv, fac, gain, ld, b_own, b_in, w_last,
    load_sem, tot_sem, a2a_sem, perm_send, perm_recv, fwd_send, fwd_recv, tp_sem, b_sem,
):
    z, y, x = (lax.axis_index(a) for a in SEQ)
    me = z * 8 + y * 2 + x
    tp = lax.axis_index("tp")
    sibling = {"tp": 1 - tp}
    across = {"pp": 1 - lax.axis_index("pp")}

    zs = [lax.rem(z + d, 4) for d in range(4)]
    ys = [lax.rem(y + d, 4) for d in range(4)]
    xs = [x, 1 - x]
    peers = [
        (zs[i] * 8 + ys[j] * 2 + xs[k], {"seq_0": zs[i], "seq_1": ys[j], "seq_2": xs[k]})
        for i in range(4)
        for j in range(4)
        for k in range(2)
    ][1:]

    mark("loads")
    loads = []

    def load(src, dst):
        copy = pltpu.make_async_copy(src, dst, load_sem.at[len(loads)])
        copy.start()
        loads.append(copy)
        return copy

    ld_load = load(ld_hbm.at[0], ld)
    k_load = load(k_hbm.at[0], k)
    v_load = load(v_hbm.at[0], v)
    q_load = load(q_hbm.at[0], q)
    gain_load = load(gain_hbm, gain)
    w_loads = []
    for j in (0, 2, 4, 6, 8, 10, 11):
        wide = CW if j >= CHUNKS - 2 else 2 * CW
        for part, side in enumerate((tp, 1 - tp)):
            at = pl.multiple_of(side * (MODEL // 2) + j * CW, CW)
            w_loads.append(
                load(w_hbm.at[0, :, pl.ds(at, wide)], w.at[:, pl.ds(place(j, part), wide)])
            )

    mark("barrier")
    barrier = pltpu.get_barrier_semaphore()

    for _, device in peers:
        pl.semaphore_signal(barrier, inc=1, device_id=device, device_id_type=MESH)
    pl.semaphore_signal(barrier, inc=1, device_id=sibling, device_id_type=MESH)
    pl.semaphore_signal(barrier, inc=1, device_id=across, device_id_type=MESH)
    pl.semaphore_wait(barrier, BLOCKS + 1)

    def permute(j):
        return pltpu.make_async_remote_copy(
            src_ref=up_hbm.at[0, :, pl.ds(j * CW, CW)],
            dst_ref=up.at[:, pl.ds(place(j, 0), CW)],
            send_sem=perm_send.at[j],
            recv_sem=perm_recv.at[j],
            device_id=across,
            device_id_type=MESH,
        )

    def forward(j):
        return pltpu.make_async_remote_copy(
            src_ref=up.at[:, pl.ds(place(j, 0), CW)],
            dst_ref=up.at[:, pl.ds(place(j, 1), CW)],
            send_sem=fwd_send.at[j],
            recv_sem=fwd_recv.at[j],
            device_id=sibling,
            device_id_type=MESH,
        )

    def exchange(src, dst, send_sem, recv_sem):
        for p, device in peers:
            pltpu.make_async_remote_copy(
                src_ref=src.at[p],
                dst_ref=dst.at[me],
                send_sem=send_sem,
                recv_sem=recv_sem,
                device_id=device,
                device_id_type=MESH,
            ).start()
        dst[me] = src[me]

    def arrived(ref, sem):
        whole = ref.at[pl.ds(0, BLOCKS - 1)]
        pltpu.make_async_copy(whole, whole, sem).wait()

    mark("perm01")
    for j in (0, 1):
        permute(j).start()

    ld_load.wait()
    mark("cumsum")
    cum = ld[...]
    column_of = lax.broadcasted_iota(jnp.int32, (HEADS, TOK), 1)
    step = 1
    while step < TOK:
        moved = pltpu.roll(cum, step, 1)
        cum = cum + jnp.where(column_of >= step, moved, 0.0)
        step *= 2
    crow[...] = cum
    total = jnp.broadcast_to(cum[:, TOK - 1 : TOK], (HEADS, HEAD))
    for h in range(HEADS):
        totals[2 * h : 2 * h + 1, 0] = total[h : h + 1]
        totals[2 * h + 1 : 2 * h + 2, 0] = total[h : h + 1]
    mark("ccol")
    turned = cum.T
    for h in range(HEADS):
        ccol[h] = jnp.broadcast_to(turned[:, h : h + 1], (TOK, HEAD))

    mark("kvwait")
    k_load.wait()
    v_load.wait()

    mark("localstate")
    @pl.loop(0, HEADS, unroll=4)
    def _(h):
        tail = jnp.exp(totals[2 * h] - ccol[h])
        tails[h] = tail
        weighted = (k[:, lanes(h)].astype(F32) * tail).astype(BF)
        local_state = nn(weighted.T, v[:, lanes(h)]).astype(BF)
        own_f[2 * h] = local_state[:ROWS]
        own_f[2 * h + 1] = local_state[ROWS:]

    mark("a2a_f1_send")
    exchange(own_f, got_f, a2a_sem.at[0], a2a_sem.at[1])
    exchange(totals, tot_in, tot_sem.at[0], tot_sem.at[1])
    for j in (2, 3, 4):
        permute(j).start()
    q_load.wait()

    mark("intra")
    lower = lax.broadcasted_iota(jnp.int32, (HALF, HALF), 0) >= lax.broadcasted_iota(
        jnp.int32, (HALF, HALF), 1
    )
    upper = lax.broadcasted_iota(jnp.int32, (HALF, HALF), 0) <= lax.broadcasted_iota(
        jnp.int32, (HALF, HALF), 1
    )
    low = -1e30

    def decay_parts(h):
        col = ccol[h]
        col2 = jnp.concatenate([col, col], axis=1)
        row = crow[pl.ds(h, 1), :]
        c0, c1 = col2[:HALF], col2[HALF:]
        r0, r1 = row[:, :HALF], row[:, HALF:]
        d00 = jnp.exp(jnp.where(lower, c0 - r0, low))
        d10 = jnp.exp(c1 - r0)
        d11 = jnp.exp(jnp.where(lower, c1 - r1, low))
        return d00, d10, d11

    def turned_parts(h):
        col = ccol[h]
        col2 = jnp.concatenate([col, col], axis=1)
        row = crow[pl.ds(h, 1), :]
        c0, c1 = col2[:HALF], col2[HALF:]
        r0, r1 = row[:, :HALF], row[:, HALF:]
        t00 = jnp.exp(jnp.where(upper, r0 - c0, low))
        t01 = jnp.exp(r1 - c0)
        t11 = jnp.exp(jnp.where(upper, r1 - c1, low))
        return t00, t01, t11

    @pl.loop(0, HEADS)
    def _(h):
        qh, kh, vh = q[:, lanes(h)], k[:, lanes(h)], v[:, lanes(h)]
        q0, q1, k0, k1 = qh[:HALF], qh[HALF:], kh[:HALF], kh[HALF:]
        d00, d10, d11 = decay_parts(h)
        m00 = (nt(q0, k0) * d00).astype(BF)
        m10 = (nt(q1, k0) * d10).astype(BF)
        m11 = (nt(q1, k1) * d11).astype(BF)
        att[:HALF, lanes(h)] = nn(m00, vh[:HALF])
        att[HALF:, lanes(h)] = nn(jnp.concatenate([m10, m11], axis=1), vh)
        t00, t01, t11 = turned_parts(h)
        mta[h, :, :HALF] = (nt(k0, q0) * t00).astype(BF)
        mta[h, :, HALF:] = (nt(k0, q1) * t01).astype(BF)
        mtb[h] = (nt(k1, q1) * t11).astype(BF)
        wq = (qh.astype(F32) * jnp.exp(ccol[h])).astype(BF)
        wqt[h] = wq.T

    mark("wait_f1")
    arrived(tot_in, tot_sem.at[1])
    arrived(got_f, a2a_sem.at[1])
    mark("scan_f")
    running = jnp.zeros((ROWS, HEAD), F32)
    for b in range(BLOCKS):
        scan_f[b] = running.astype(BF)
        running = jnp.exp(tot_in[b]) * running + got_f[b].astype(F32)
    mark("a2a_f2_send")
    exchange(scan_f, state, a2a_sem.at[2], a2a_sem.at[3])
    for j in range(5, CHUNKS):
        permute(j).start()

    mark("wload")
    gain_load.wait()
    for copy in w_loads:
        copy.wait()

    def hidden(start, depth, first):
        @pl.loop(0, 4)
        def _(n):
            at = pl.ds(pl.multiple_of(n * 512, 512), 512)
            part = nt(up[:, start : start + depth], w[at, start : start + depth])
            if first:
                gh[:, at] = part
            else:
                gh[:, at] += part

    def relay(*chunks):
        for j in chunks:
            permute(j).wait_recv()
            forward(j).start()

    def relayed(*chunks):
        for j in chunks:
            forward(j).wait_recv()

    @pl.loop(0, HEADS)
    def _(h):
        scale = jnp.broadcast_to(gain[:, lanes(h)], (HEAD, HEAD)).T
        w_last[lanes(h), :] = (w[lanes(h), MODEL - CW :].astype(F32) * scale).astype(BF)

    mark("relay012")
    relay(0, 1, 2, 3)
    relayed(0, 1)
    mark("hidden01")
    hidden(0, 512, True)
    mark("relay23")
    relay(4)
    relayed(2, 3)
    mark("hidden23")
    hidden(512, 512, False)

    mark("wait_f2")
    arrived(state, a2a_sem.at[3])
    mark("att_inter")
    sq_own[...] = jnp.zeros_like(sq_own)

    @pl.loop(0, HEADS // 2, unroll=2)
    def _(i):
        at = pair_lanes(i)
        new = att[:, at] + jnp.exp(two_columns(ccol, i)) * nn(q[:, at], two_states(state, i))
        att[:, at] = new
        ga[:, at] = (new * gain[:, at]).astype(BF)
        both = new * new
        sq_own[...] += both[:, :HEAD] + both[:, HEAD:]

    def to_sibling(src, dst, i):
        return pltpu.make_async_remote_copy(
            src_ref=src,
            dst_ref=dst,
            send_sem=tp_sem.at[2 * i],
            recv_sem=tp_sem.at[2 * i + 1],
            device_id=sibling,
            device_id_type=MESH,
        )

    def tail_product():
        b_own[...] = nn(ga[...], w[:, 2560:]).astype(BF)
        for at in range(0, 4 * CW, CW):
            copy = pltpu.make_async_remote_copy(
                src_ref=b_own.at[:, pl.ds(at, CW)],
                dst_ref=b_in.at[:, pl.ds(at + CW if at % (2 * CW) == 0 else at - CW, CW)],
                send_sem=b_sem.at[0],
                recv_sem=b_sem.at[1],
                device_id=sibling,
                device_id_type=MESH,
            )
            copy.start()

    squares = to_sibling(sq_own, sq_in, 0)
    squares.start()
    cr_own[...] = jnp.zeros_like(cr_own)
    mark("tail_product")
    tail_product()
    mark("relay45")
    relay(5)
    relayed(4, 5)
    mark("hidden45")
    hidden(1024, 512, False)
    mark("inverse")
    squares.wait_recv()
    square_total = jnp.sum(sq_own[...] + sq_in[...], axis=1, keepdims=True)
    inv[...] = jnp.broadcast_to(1.0 / jnp.sqrt(square_total / FEATURES + EPS), (TOK, HEAD))
    mark("relay67")
    relay(6, 7)
    relayed(6, 7)
    mark("hidden67")
    hidden(1536, 512, False)
    mark("relay89")
    relay(8, 9)
    relayed(8, 9)
    mark("hidden89")

    @pl.loop(0, 4)
    def _(n):
        at = pl.ds(pl.multiple_of(n * 512, 512), 512)
        new = gh[:, at] + nt(up[:, 2048:2560], w[at, 2048:2560])
        gh[:, at] = new
        both = new * gain[:, at] * att[:, at]
        cr_own[...] += (both[:, :128] + both[:, 128:256]) + (both[:, 256:384] + both[:, 384:])

    crossed = to_sibling(cr_own, cr_in, 1)
    crossed.start()
    mark("relay10")
    relay(10)
    mark("own10")
    hidden(2560, 128, False)
    pltpu.make_async_copy(b_in, b_in, b_sem.at[1]).wait()
    crossed.wait_recv()
    mark("relay11")
    relay(11)
    relayed(10)
    mark("sib10own11")

    @pl.loop(0, 4)
    def _(n):
        at = pl.ds(pl.multiple_of(n * 512, 512), 512)
        new = gh[:, at] + nt(up[:, 2688:2944], w[at, 2688:2944])
        inverse = inv[...]
        gh[:, at] = new * gain[:, at] * jnp.concatenate([inverse] * 4, axis=1)

    crossed.wait_send()
    part = cr_own[...] + cr_in[...]
    for at in range(0, 3 * CW, CW):
        both = b_own[:, at : at + CW].astype(F32) + b_in[:, at : at + CW].astype(F32)
        part += up[:, 2560 + at : 2560 + at + CW].astype(F32) * both
    cr_own[...] = part
    mark("relayed11")
    relayed(11)
    mark("crossing11")
    both = b_own[:, 3 * CW :].astype(F32) + b_in[:, 3 * CW :].astype(F32)
    part = cr_own[...] + up[:, MODEL - CW :].astype(F32) * both
    cross_total = jnp.sum(part, axis=1, keepdims=True)
    inverse = inv[...]
    fac[...] = inverse * inverse * inverse * jnp.broadcast_to(cross_total / FEATURES, (TOK, HEAD))
    up_last = (up[:, MODEL - CW :].astype(F32) * inverse).astype(BF)

    mark("ga_passed")
    low_rows, high_rows = pl.ds(0, ROWS // 2), pl.ds(ROWS // 2, ROWS // 2)

    def send_piece(src, dst, p, device, rows, sem):
        pltpu.make_async_remote_copy(
            src_ref=src.at[p, rows],
            dst_ref=dst.at[me, rows],
            send_sem=a2a_sem.at[sem],
            recv_sem=a2a_sem.at[sem + 1],
            device_id=device,
            device_id_type=MESH,
        ).start()

    def piece_arrived(ref, rows, sem):
        whole = ref.at[pl.ds(0, BLOCKS - 1), rows]
        pltpu.make_async_copy(whole, whole, a2a_sem.at[sem]).wait()

    def last_step(n):
        at = pl.ds(pl.multiple_of(zs[n] * 512, 512), 512)
        gh[:, at] += nt(up_last, w_last[at, :])

    def passing(n):
        for j in range(4):
            h = 4 * zs[n] + j
            grad = (gh[:, lanes(h)] - fac[...] * att[:, lanes(h)]).astype(BF)
            ga[:, lanes(h)] = grad
            passed = nn(wqt[h], grad).astype(BF)
            own_b[2 * h] = passed[:ROWS]
            own_b[2 * h + 1] = passed[ROWS:]

    def send_low(part):
        for p, device in part:
            send_piece(own_b, got_b, p, device, low_rows, 4)

    last_step(0)
    last_step(1)
    passing(0)
    passing(1)
    last_step(2)
    last_step(3)
    send_low(peers[:15])
    passing(2)
    passing(3)
    send_low(peers[15:])
    mark("send_high")
    for p, device in peers:
        send_piece(own_b, got_b, p, device, high_rows, 6)
    got_b[me] = own_b[me]

    def gradients(i):
        two = pair_lanes(i)
        inter = jnp.exp(two_columns(ccol, i)) * nt(ga[:, two], two_states(state, i))
        for side in (0, 1):
            h = 2 * i + side
            qh, kh, vh, gah = q[:, lanes(h)], k[:, lanes(h)], v[:, lanes(h)], ga[:, lanes(h)]
            v0, v1, g0, g1 = vh[:HALF], vh[HALF:], gah[:HALF], gah[HALF:]
            d00, d10, d11 = decay_parts(h)
            m00 = (nt(g0, v0) * d00).astype(BF)
            m10 = (nt(g1, v0) * d10).astype(BF)
            m11 = (nt(g1, v1) * d11).astype(BF)
            dq0 = nn(m00, kh[:HALF])
            dq1 = nn(jnp.concatenate([m10, m11], axis=1), kh)
            more = inter[:, side * HEAD : (side + 1) * HEAD]
            dqs[:HALF, lanes(h)] = (dq0 + more[:HALF]).astype(BF)
            dqs[HALF:, lanes(h)] = (dq1 + more[HALF:]).astype(BF)
            t00, t01, t11 = turned_parts(h)
            n0 = jnp.concatenate(
                [(nt(v0, g0) * t00).astype(BF), (nt(v0, g1) * t01).astype(BF)], axis=1
            )
            n1 = (nt(v1, g1) * t11).astype(BF)
            att[:HALF, lanes(h)] = nn(n0, qh)
            att[HALF:, lanes(h)] = nn(n1, qh[HALF:])
            gh[:HALF, lanes(h)] = nn(mta[h], gah)
            gh[HALF:, lanes(h)] = nn(mtb[h], g1)

    def scan_back(rows):
        running = jnp.zeros((ROWS // 2, HEAD), F32)
        for b in reversed(range(BLOCKS)):
            scan_b[b, rows] = running.astype(BF)
            running = jnp.exp(tot_in[b]) * running + got_b[b, rows].astype(F32)
        for p, device in peers:
            send_piece(scan_b, later, p, device, rows, 8 if rows is low_rows else 10)
        later[me, rows] = scan_b[me, rows]

    mark("grad1")
    pl.loop(0, 3)(gradients)
    mark("wait_b1a")
    piece_arrived(got_b, low_rows, 5)
    mark("scan_ba")
    scan_back(low_rows)
    mark("grad2")
    pl.loop(3, 5)(gradients)
    mark("wait_b1b")
    piece_arrived(got_b, high_rows, 7)
    mark("scan_bb")
    scan_back(high_rows)
    mark("grad3")
    pl.loop(5, HEADS // 2)(gradients)
    mark("wait_b2")
    piece_arrived(later, low_rows, 9)
    piece_arrived(later, high_rows, 11)

    mark("sendwaits")
    arrived(totals, tot_sem.at[0])
    arrived(own_f, a2a_sem.at[0])
    arrived(scan_f, a2a_sem.at[2])
    for rows, sem in ((low_rows, 4), (high_rows, 6)):
        piece_arrived(own_b, rows, sem)
        piece_arrived(scan_b, rows, sem + 4)
    pltpu.make_async_copy(b_own, b_own, b_sem.at[0]).wait()
    for j in range(CHUNKS):
        permute(j).wait_send()
        forward(j).wait_send()
    squares.wait_send()
    mark(None)


def finish(
    dqs, att, gh, k, v, later, tails, dq_hbm, dk_hbm, dv_hbm, dks, dvs, out_sem
):
    pltpu.make_async_copy(dqs, dq_hbm.at[0], out_sem.at[0]).start()

    def put(src, dst, at, i):
        pltpu.make_async_copy(src.at[:, at], dst.at[0, :, at], out_sem.at[i]).start()

    @pl.loop(0, HEADS // 4)
    def _(n):
        for i in (2 * n, 2 * n + 1):
            at = pair_lanes(i)
            lt = two_states(later, i)
            tail = two_columns(tails, i)
            dks[:, at] = (att[:, at] + tail * nt(v[:, at], lt)).astype(BF)
            dvs[:, at] = (gh[:, at] + tail * nn(k[:, at], lt)).astype(BF)
        four = pl.ds(pl.multiple_of(n * 512, 512), 512)
        put(dks, dk_hbm, four, 1)
        put(dvs, dv_hbm, four, 2)

    for i, (src, dst) in enumerate(((dqs, dq_hbm), (dks, dk_hbm), (dvs, dv_hbm))):
        pltpu.make_async_copy(src, dst.at[0], out_sem.at[i]).wait()


def local(queries, keys, values, upstream, out_weight, gain, log_decay):
    vmem = pltpu.VMEM
    piece = vmem((BLOCKS, ROWS, HEAD), BF)
    column = vmem((TOK, HEAD), F32)
    rows_bf = vmem((TOK, WIDTH), BF)
    rows_f32 = vmem((TOK, WIDTH), F32)
    columns = vmem((HEADS, TOK, HEAD), F32)
    totals = vmem((BLOCKS, 1, HEAD), F32)
    dma = pltpu.SemaphoreType.DMA
    hbm = pl.BlockSpec(memory_space=pl.ANY)
    here = pl.BlockSpec(memory_space=vmem)
    kept = pl.pallas_call(
        kernel,
        out_shape=(rows_bf, rows_f32, rows_f32, rows_bf, rows_bf, piece, columns),
        in_specs=[hbm] * 7,
        out_specs=[here] * 7,
        scratch_shapes=[
            columns,
            totals,
            rows_bf,
            vmem((WIDTH, MODEL), BF),
            vmem((TOK, MODEL), BF),
            rows_bf,
            vmem((HEADS, HEAD, TOK), BF),
            vmem((HEADS, TOK), F32),
            vmem((HEADS, HALF, TOK), BF),
            vmem((HEADS, HALF, HALF), BF),
            piece, piece, piece, piece, piece, piece, piece,
            totals,
            column, column, column, column, column, column,
            vmem((1, WIDTH), F32),
            vmem((HEADS, TOK), F32),
            vmem((TOK, 4 * CW), BF),
            vmem((TOK, 4 * CW), BF),
            vmem((WIDTH, CW), BF),
            dma((19,)),
            dma((2,)),
            dma((12,)),
            dma((CHUNKS,)), dma((CHUNKS,)), dma((CHUNKS,)), dma((CHUNKS,)),
            dma((4,)),
            dma((2,)),
        ],
        compiler_params=pltpu.CompilerParams(
            collective_id=0, has_side_effects=True, vmem_limit_bytes=45 << 20
        ),
        name="decayed_backward",
    )(queries, keys, values, upstream, out_weight, gain, log_decay)
    out = jax.ShapeDtypeStruct((1, TOK, WIDTH), BF)
    return pl.pallas_call(
        finish,
        out_shape=(out, out, out),
        in_specs=[here] * 7,
        out_specs=[hbm] * 3,
        scratch_shapes=[rows_bf, rows_bf, dma((3,))],
        compiler_params=pltpu.CompilerParams(vmem_limit_bytes=24 << 20),
        name="finish",
    )(*kept)


def solution(mesh):
    torus = Mesh(
        mesh.devices.reshape(4, 4, 2, mesh.shape["tp"], mesh.shape["pp"]),
        ("seq_0", "seq_1", "seq_2", "tp", "pp"),
    )
    rows = P("pp", SEQ, "tp")
    placed = (rows, rows, rows, rows, P("pp", "tp", None), P("pp", "tp"), P("pp", "tp", SEQ))
    return jax.shard_map(
        local, mesh=torus, in_specs=placed, out_specs=(rows, rows, rows), check_vma=False
    )
```

```python
import jax
import jax.numpy as jnp
from jax import lax
from jax.experimental import pallas as pl
from jax.experimental.pallas import tpu as pltpu
from jax.sharding import Mesh
from jax.sharding import PartitionSpec as P

HEAD = 128
SEQ = ("seq_0", "seq_1", "seq_2")
MESH = pl.DeviceIdType.MESH
EPS = 1e-06
BF = jnp.bfloat16
F32 = jnp.float32

TOK = 512
HALF = 256
WIDTH = 2048
HEADS = 16
MODEL = 3072
CHUNKS = 12
CW = 128
BLOCKS = 32
ROWS = 64
FEATURES = 4096


def mark(name):
    pass


def nn(a, b):
    return lax.dot_general(a, b, (((1,), (0,)), ((), ())), preferred_element_type=F32)


def nt(a, b):
    return lax.dot_general(a, b, (((1,), (1,)), ((), ())), preferred_element_type=F32)


def lanes(h):
    return pl.ds(pl.multiple_of(h * HEAD, HEAD), HEAD)


def pair_lanes(i):
    if isinstance(i, int):
        return pl.ds(i * 2 * HEAD, 2 * HEAD)
    return pl.ds(pl.multiple_of(i * 2 * HEAD, 2 * HEAD), 2 * HEAD)


def two_states(ref, i):
    none = jnp.zeros((HEAD, HEAD), BF)
    first = jnp.concatenate([ref[4 * i], ref[4 * i + 1]], axis=0)
    second = jnp.concatenate([ref[4 * i + 2], ref[4 * i + 3]], axis=0)
    return jnp.concatenate(
        [jnp.concatenate([first, none], axis=1), jnp.concatenate([none, second], axis=1)], axis=0
    )


def two_columns(ref, i):
    return jnp.concatenate([ref[2 * i], ref[2 * i + 1]], axis=1)


def place(c, part):
    if c < CHUNKS - 2:
        return c // 2 * 4 * CW + part * 2 * CW + c % 2 * CW
    return (2 * c + part) * CW


def kernel(
    q_hbm, k_hbm, v_hbm, up_hbm, w_hbm, gain_hbm, ld_hbm,
    dqs, att, gh, k, v, later, tails,
    ccol, totals, q, w, up, ga, wqt, crow, mta, mtb,
    own_f, got_f, scan_f, state, own_b, got_b, scan_b,
    tot_in, sq_own, sq_in, cr_own, cr_in, inv, fac, gain, ld, b_own, b_in, w_last, up_from,
    load_sem, tot_sem, a2a_sem, perm_send, perm_recv, fwd_send, fwd_recv, tp_sem, b_sem,
):
    z, y, x = (lax.axis_index(a) for a in SEQ)
    me = z * 8 + y * 2 + x
    tp = lax.axis_index("tp")
    sibling = {"tp": 1 - tp}
    across = {"pp": 1 - lax.axis_index("pp")}

    zs = [lax.rem(z + d, 4) for d in range(4)]
    ys = [lax.rem(y + d, 4) for d in range(4)]
    xs = [x, 1 - x]
    def hops(at):
        return min(at[0], 4 - at[0]) + min(at[1], 4 - at[1]) + at[2]

    offsets = [(i, j, k) for i in range(4) for j in range(4) for k in range(2)][1:]
    offsets.sort(key=hops, reverse=True)

    def peer(at):
        i, j, k = at
        device = {"seq_0": zs[i], "seq_1": ys[j], "seq_2": xs[k]}
        return zs[i] * 8 + ys[j] * 2 + xs[k], device

    peers = [peer(at) for at in offsets]

    mark("loads")
    loads = []

    def load(src, dst):
        copy = pltpu.make_async_copy(src, dst, load_sem.at[len(loads)])
        copy.start()
        loads.append(copy)
        return copy

    first, rest = pl.ds(0, 2 * CW), pl.ds(2 * CW, MODEL // 2 - 2 * CW)
    up_loads = [load(up_hbm.at[0, :, cols], up_from.at[:, cols]) for cols in (first, rest)]
    ld_load = load(ld_hbm.at[0], ld)
    k_load = load(k_hbm.at[0], k)
    v_load = load(v_hbm.at[0], v)
    q_load = load(q_hbm.at[0], q)
    gain_load = load(gain_hbm, gain)
    w_loads = []
    for j in (0, 2, 4, 6, 8, 10, 11):
        wide = CW if j >= CHUNKS - 2 else 2 * CW
        for part, side in enumerate((tp, 1 - tp)):
            at = pl.multiple_of(side * (MODEL // 2) + j * CW, CW)
            w_loads.append(
                load(w_hbm.at[0, :, pl.ds(at, wide)], w.at[:, pl.ds(place(j, part), wide)])
            )

    mark("barrier")
    barrier = pltpu.get_barrier_semaphore()

    for _, device in peers:
        pl.semaphore_signal(barrier, inc=1, device_id=device, device_id_type=MESH)
    pl.semaphore_signal(barrier, inc=1, device_id=sibling, device_id_type=MESH)
    pl.semaphore_signal(barrier, inc=1, device_id=across, device_id_type=MESH)
    pl.semaphore_wait(barrier, BLOCKS + 1)

    def permute(j):
        return pltpu.make_async_remote_copy(
            src_ref=up_from.at[:, pl.ds(j * CW, CW)],
            dst_ref=up.at[:, pl.ds(place(j, 0), CW)],
            send_sem=perm_send.at[j],
            recv_sem=perm_recv.at[j],
            device_id=across,
            device_id_type=MESH,
        )

    def forward(j):
        return pltpu.make_async_remote_copy(
            src_ref=up.at[:, pl.ds(place(j, 0), CW)],
            dst_ref=up.at[:, pl.ds(place(j, 1), CW)],
            send_sem=fwd_send.at[j],
            recv_sem=fwd_recv.at[j],
            device_id=sibling,
            device_id_type=MESH,
        )

    def exchange(src, dst, send_sem, recv_sem):
        for p, device in peers:
            pltpu.make_async_remote_copy(
                src_ref=src.at[p],
                dst_ref=dst.at[me],
                send_sem=send_sem,
                recv_sem=recv_sem,
                device_id=device,
                device_id_type=MESH,
            ).start()
        dst[me] = src[me]

    def arrived(ref, sem):
        whole = ref.at[pl.ds(0, BLOCKS - 1)]
        pltpu.make_async_copy(whole, whole, sem).wait()

    mark("perm01")
    up_loads[0].wait()
    for j in (0, 1):
        permute(j).start()

    ld_load.wait()
    mark("cumsum")
    cum = ld[...]
    column_of = lax.broadcasted_iota(jnp.int32, (HEADS, TOK), 1)
    step = 1
    while step < TOK:
        moved = pltpu.roll(cum, step, 1)
        cum = cum + jnp.where(column_of >= step, moved, 0.0)
        step *= 2
    crow[...] = cum
    total = jnp.broadcast_to(cum[:, TOK - 1 : TOK], (HEADS, HEAD))
    for h in range(HEADS):
        totals[2 * h : 2 * h + 1, 0] = total[h : h + 1]
        totals[2 * h + 1 : 2 * h + 2, 0] = total[h : h + 1]
    mark("ccol")
    turned = cum.T
    for h in range(HEADS):
        ccol[h] = jnp.broadcast_to(turned[:, h : h + 1], (TOK, HEAD))

    mark("kvwait")
    k_load.wait()
    v_load.wait()

    mark("localstate")
    @pl.loop(0, HEADS, unroll=4)
    def _(h):
        tail = jnp.exp(totals[2 * h] - ccol[h])
        tails[h] = tail
        weighted = (k[:, lanes(h)].astype(F32) * tail).astype(BF)
        local_state = nn(weighted.T, v[:, lanes(h)]).astype(BF)
        own_f[2 * h] = local_state[:ROWS]
        own_f[2 * h + 1] = local_state[ROWS:]

    mark("a2a_f1_send")
    exchange(own_f, got_f, a2a_sem.at[0], a2a_sem.at[1])
    exchange(totals, tot_in, tot_sem.at[0], tot_sem.at[1])
    up_loads[1].wait()
    for j in (2, 3, 4):
        permute(j).start()
    q_load.wait()

    mark("intra")
    lower = lax.broadcasted_iota(jnp.int32, (HALF, HALF), 0) >= lax.broadcasted_iota(
        jnp.int32, (HALF, HALF), 1
    )
    upper = lax.broadcasted_iota(jnp.int32, (HALF, HALF), 0) <= lax.broadcasted_iota(
        jnp.int32, (HALF, HALF), 1
    )
    low = -1e30

    def decay_parts(h):
        col = ccol[h]
        col2 = jnp.concatenate([col, col], axis=1)
        row = crow[pl.ds(h, 1), :]
        c0, c1 = col2[:HALF], col2[HALF:]
        r0, r1 = row[:, :HALF], row[:, HALF:]
        d00 = jnp.exp(jnp.where(lower, c0 - r0, low))
        d10 = jnp.exp(c1 - r0)
        d11 = jnp.exp(jnp.where(lower, c1 - r1, low))
        return d00, d10, d11

    def turned_parts(h):
        col = ccol[h]
        col2 = jnp.concatenate([col, col], axis=1)
        row = crow[pl.ds(h, 1), :]
        c0, c1 = col2[:HALF], col2[HALF:]
        r0, r1 = row[:, :HALF], row[:, HALF:]
        t00 = jnp.exp(jnp.where(upper, r0 - c0, low))
        t01 = jnp.exp(r1 - c0)
        t11 = jnp.exp(jnp.where(upper, r1 - c1, low))
        return t00, t01, t11

    @pl.loop(0, HEADS)
    def _(h):
        qh, kh, vh = q[:, lanes(h)], k[:, lanes(h)], v[:, lanes(h)]
        q0, q1, k0, k1 = qh[:HALF], qh[HALF:], kh[:HALF], kh[HALF:]
        d00, d10, d11 = decay_parts(h)
        m00 = (nt(q0, k0) * d00).astype(BF)
        m10 = (nt(q1, k0) * d10).astype(BF)
        m11 = (nt(q1, k1) * d11).astype(BF)
        att[:HALF, lanes(h)] = nn(m00, vh[:HALF])
        att[HALF:, lanes(h)] = nn(jnp.concatenate([m10, m11], axis=1), vh)
        t00, t01, t11 = turned_parts(h)
        mta[h, :, :HALF] = (nt(k0, q0) * t00).astype(BF)
        mta[h, :, HALF:] = (nt(k0, q1) * t01).astype(BF)
        mtb[h] = (nt(k1, q1) * t11).astype(BF)
        wq = (qh.astype(F32) * jnp.exp(ccol[h])).astype(BF)
        wqt[h] = wq.T

    mark("wait_f1")
    arrived(tot_in, tot_sem.at[1])
    arrived(got_f, a2a_sem.at[1])
    mark("scan_f")
    running = jnp.zeros((ROWS, HEAD), F32)
    for b in range(BLOCKS):
        scan_f[b] = running.astype(BF)
        running = jnp.exp(tot_in[b]) * running + got_f[b].astype(F32)
    mark("a2a_f2_send")
    exchange(scan_f, state, a2a_sem.at[2], a2a_sem.at[3])
    for j in range(5, CHUNKS):
        permute(j).start()

    mark("wload")
    gain_load.wait()
    for copy in w_loads:
        copy.wait()

    def hidden(start, depth, first):
        @pl.loop(0, 4, unroll=2)
        def _(n):
            at = pl.ds(pl.multiple_of(n * 512, 512), 512)
            part = nt(up[:, start : start + depth], w[at, start : start + depth])
            if first:
                gh[:, at] = part
            else:
                gh[:, at] += part

    def relay(*chunks):
        for j in chunks:
            permute(j).wait_recv()
            forward(j).start()

    def relayed(*chunks):
        for j in chunks:
            forward(j).wait_recv()

    @pl.loop(0, HEADS, unroll=2)
    def _(h):
        turned = w[lanes(h), MODEL - CW :].astype(F32).T
        w_last[:, lanes(h)] = (turned * gain[:, lanes(h)]).astype(BF)

    mark("relay012")
    relay(0, 1, 2, 3)
    relayed(0, 1)
    mark("hidden01")
    hidden(0, 512, True)
    mark("relay23")
    relay(4)
    relayed(2, 3)
    mark("hidden23")
    hidden(512, 512, False)

    mark("wait_f2")
    arrived(state, a2a_sem.at[3])
    mark("att_inter")
    sq_own[...] = jnp.zeros_like(sq_own)

    @pl.loop(0, HEADS // 2, unroll=2)
    def _(i):
        at = pair_lanes(i)
        new = att[:, at] + jnp.exp(two_columns(ccol, i)) * nn(q[:, at], two_states(state, i))
        att[:, at] = new
        ga[:, at] = (new * gain[:, at]).astype(BF)
        both = new * new
        sq_own[...] += both[:, :HEAD] + both[:, HEAD:]

    def to_sibling(src, dst, i):
        return pltpu.make_async_remote_copy(
            src_ref=src,
            dst_ref=dst,
            send_sem=tp_sem.at[2 * i],
            recv_sem=tp_sem.at[2 * i + 1],
            device_id=sibling,
            device_id_type=MESH,
        )

    def tail_product():
        b_own[...] = nn(ga[...], w[:, 2560:]).astype(BF)
        for at in range(0, 4 * CW, CW):
            copy = pltpu.make_async_remote_copy(
                src_ref=b_own.at[:, pl.ds(at, CW)],
                dst_ref=b_in.at[:, pl.ds(at + CW if at % (2 * CW) == 0 else at - CW, CW)],
                send_sem=b_sem.at[0],
                recv_sem=b_sem.at[1],
                device_id=sibling,
                device_id_type=MESH,
            )
            copy.start()

    squares = to_sibling(sq_own, sq_in, 0)
    squares.start()
    cr_own[...] = jnp.zeros_like(cr_own)
    mark("tail_product")
    tail_product()
    mark("relay45")
    relay(5)
    relayed(4, 5)
    mark("hidden45")
    hidden(1024, 512, False)
    mark("inverse")
    squares.wait_recv()
    square_total = jnp.sum(sq_own[...] + sq_in[...], axis=1, keepdims=True)
    inv[...] = jnp.broadcast_to(1.0 / jnp.sqrt(square_total / FEATURES + EPS), (TOK, HEAD))
    mark("relay67")
    relay(6, 7)
    relayed(6, 7)
    mark("hidden67")
    hidden(1536, 512, False)
    mark("relay89")
    relay(8, 9)
    relayed(8, 9)
    mark("hidden89")

    @pl.loop(0, 4, unroll=2)
    def _(n):
        at = pl.ds(pl.multiple_of(n * 512, 512), 512)
        new = gh[:, at] + nt(up[:, 2048:2560], w[at, 2048:2560])
        gh[:, at] = new
        both = new * gain[:, at] * att[:, at]
        cr_own[...] += (both[:, :128] + both[:, 128:256]) + (both[:, 256:384] + both[:, 384:])

    crossed = to_sibling(cr_own, cr_in, 1)
    crossed.start()
    mark("relay10")
    relay(10)
    mark("own10")
    hidden(2560, 128, False)
    pltpu.make_async_copy(b_in, b_in, b_sem.at[1]).wait()
    crossed.wait_recv()
    mark("relay11")
    relay(11)
    relayed(10)
    mark("sib10own11")

    @pl.loop(0, 4, unroll=2)
    def _(n):
        at = pl.ds(pl.multiple_of(n * 512, 512), 512)
        new = gh[:, at] + nt(up[:, 2688:2944], w[at, 2688:2944])
        inverse = inv[...]
        gh[:, at] = new * gain[:, at] * jnp.concatenate([inverse] * 4, axis=1)

    crossed.wait_send()
    part = cr_own[...] + cr_in[...]
    for at in range(0, 3 * CW, CW):
        both = b_own[:, at : at + CW].astype(F32) + b_in[:, at : at + CW].astype(F32)
        part += up[:, 2560 + at : 2560 + at + CW].astype(F32) * both
    cr_own[...] = part
    mark("relayed11")
    relayed(11)
    mark("crossing11")
    both = b_own[:, 3 * CW :].astype(F32) + b_in[:, 3 * CW :].astype(F32)
    part = cr_own[...] + up[:, MODEL - CW :].astype(F32) * both
    cross_total = jnp.sum(part, axis=1, keepdims=True)
    inverse = inv[...]
    fac[...] = inverse * inverse * inverse * jnp.broadcast_to(cross_total / FEATURES, (TOK, HEAD))
    up_last = (up[:, MODEL - CW :].astype(F32) * inverse).astype(BF)

    mark("ga_passed")
    low_rows, high_rows = pl.ds(0, ROWS // 2), pl.ds(ROWS // 2, ROWS // 2)

    def send_piece(src, dst, p, device, rows, sem):
        pltpu.make_async_remote_copy(
            src_ref=src.at[p, rows],
            dst_ref=dst.at[me, rows],
            send_sem=a2a_sem.at[sem],
            recv_sem=a2a_sem.at[sem + 1],
            device_id=device,
            device_id_type=MESH,
        ).start()

    def piece_arrived(ref, rows, sem):
        whole = ref.at[pl.ds(0, BLOCKS - 1), rows]
        pltpu.make_async_copy(whole, whole, a2a_sem.at[sem]).wait()

    def passing(i):
        at = pair_lanes(i)
        both = gh[:, at] + nn(up_last, w_last[:, at])
        factor = fac[...]
        both = both - jnp.concatenate([factor, factor], axis=1) * att[:, at]
        both = both.astype(BF)
        ga[:, at] = both
        for side in (0, 1):
            h = 2 * i + side
            passed = nn(wqt[h], both[:, side * HEAD : (side + 1) * HEAD]).astype(BF)
            own_b[2 * h] = passed[:ROWS]
            own_b[2 * h + 1] = passed[ROWS:]

    for group in ((2, 1), (3, 0)):
        for n in group:
            passing(2 * zs[n])
            passing(2 * zs[n] + 1)
        for p, device in (peer(at) for at in offsets if at[0] in group):
            send_piece(own_b, got_b, p, device, low_rows, 4)
    mark("send_high")
    for p, device in peers:
        send_piece(own_b, got_b, p, device, high_rows, 6)
    got_b[me] = own_b[me]

    def gradients(i):
        two = pair_lanes(i)
        inter = jnp.exp(two_columns(ccol, i)) * nt(ga[:, two], two_states(state, i))
        for side in (0, 1):
            h = 2 * i + side
            qh, kh, vh, gah = q[:, lanes(h)], k[:, lanes(h)], v[:, lanes(h)], ga[:, lanes(h)]
            v0, v1, g0, g1 = vh[:HALF], vh[HALF:], gah[:HALF], gah[HALF:]
            d00, d10, d11 = decay_parts(h)
            m00 = (nt(g0, v0) * d00).astype(BF)
            m10 = (nt(g1, v0) * d10).astype(BF)
            m11 = (nt(g1, v1) * d11).astype(BF)
            dq0 = nn(m00, kh[:HALF])
            dq1 = nn(jnp.concatenate([m10, m11], axis=1), kh)
            more = inter[:, side * HEAD : (side + 1) * HEAD]
            dqs[:HALF, lanes(h)] = (dq0 + more[:HALF]).astype(BF)
            dqs[HALF:, lanes(h)] = (dq1 + more[HALF:]).astype(BF)
            t00, t01, t11 = turned_parts(h)
            n0 = jnp.concatenate(
                [(nt(v0, g0) * t00).astype(BF), (nt(v0, g1) * t01).astype(BF)], axis=1
            )
            n1 = (nt(v1, g1) * t11).astype(BF)
            att[:HALF, lanes(h)] = nn(n0, qh)
            att[HALF:, lanes(h)] = nn(n1, qh[HALF:])
            gh[:HALF, lanes(h)] = nn(mta[h], gah)
            gh[HALF:, lanes(h)] = nn(mtb[h], g1)

    def scan_back(rows):
        running = jnp.zeros((ROWS // 2, HEAD), F32)
        for b in reversed(range(BLOCKS)):
            scan_b[b, rows] = running.astype(BF)
            running = jnp.exp(tot_in[b]) * running + got_b[b, rows].astype(F32)
        for p, device in peers:
            send_piece(scan_b, later, p, device, rows, 8 if rows is low_rows else 10)
        later[me, rows] = scan_b[me, rows]

    mark("grad1")
    pl.loop(0, 3)(gradients)
    mark("wait_b1a")
    piece_arrived(got_b, low_rows, 5)
    mark("scan_ba")
    scan_back(low_rows)
    mark("grad2")
    pl.loop(3, 4)(gradients)
    mark("wait_b1b")
    piece_arrived(got_b, high_rows, 7)
    mark("scan_bb")
    scan_back(high_rows)
    mark("grad3")
    pl.loop(4, HEADS // 2)(gradients)
    mark("wait_b2")
    piece_arrived(later, low_rows, 9)
    piece_arrived(later, high_rows, 11)

    mark("sendwaits")
    arrived(totals, tot_sem.at[0])
    arrived(own_f, a2a_sem.at[0])
    arrived(scan_f, a2a_sem.at[2])
    for rows, sem in ((low_rows, 4), (high_rows, 6)):
        piece_arrived(own_b, rows, sem)
        piece_arrived(scan_b, rows, sem + 4)
    pltpu.make_async_copy(b_own, b_own, b_sem.at[0]).wait()
    for j in range(CHUNKS):
        permute(j).wait_send()
        forward(j).wait_send()
    squares.wait_send()
    mark(None)


def finish(
    dqs, att, gh, k, v, later, tails, dq_hbm, dk_hbm, dv_hbm, dks, dvs, out_sem
):
    pltpu.make_async_copy(dqs, dq_hbm.at[0], out_sem.at[0]).start()

    def put(src, dst, at, i):
        pltpu.make_async_copy(src.at[:, at], dst.at[0, :, at], out_sem.at[i]).start()

    for i in range(HEADS // 2):
        at = pair_lanes(i)
        lt = two_states(later, i)
        tail = two_columns(tails, i)
        dks[:, at] = (att[:, at] + tail * nt(v[:, at], lt)).astype(BF)
        dvs[:, at] = (gh[:, at] + tail * nn(k[:, at], lt)).astype(BF)
        if i % 2 == 1:
            part = pl.ds((i - 1) * 2 * HEAD, 4 * HEAD)
            put(dks, dk_hbm, part, 1)
            put(dvs, dv_hbm, part, 2)

    for i, (src, dst) in enumerate(((dqs, dq_hbm), (dks, dk_hbm), (dvs, dv_hbm))):
        pltpu.make_async_copy(src, dst.at[0], out_sem.at[i]).wait()


def local(queries, keys, values, upstream, out_weight, gain, log_decay):
    vmem = pltpu.VMEM
    piece = vmem((BLOCKS, ROWS, HEAD), BF)
    column = vmem((TOK, HEAD), F32)
    rows_bf = vmem((TOK, WIDTH), BF)
    rows_f32 = vmem((TOK, WIDTH), F32)
    columns = vmem((HEADS, TOK, HEAD), F32)
    totals = vmem((BLOCKS, 1, HEAD), F32)
    dma = pltpu.SemaphoreType.DMA
    hbm = pl.BlockSpec(memory_space=pl.ANY)
    here = pl.BlockSpec(memory_space=vmem)
    kept = pl.pallas_call(
        kernel,
        out_shape=(rows_bf, rows_f32, rows_f32, rows_bf, rows_bf, piece, columns),
        in_specs=[hbm] * 7,
        out_specs=[here] * 7,
        scratch_shapes=[
            columns,
            totals,
            rows_bf,
            vmem((WIDTH, MODEL), BF),
            vmem((TOK, MODEL), BF),
            rows_bf,
            vmem((HEADS, HEAD, TOK), BF),
            vmem((HEADS, TOK), F32),
            vmem((HEADS, HALF, TOK), BF),
            vmem((HEADS, HALF, HALF), BF),
            piece, piece, piece, piece, piece, piece, piece,
            totals,
            column, column, column, column, column, column,
            vmem((1, WIDTH), F32),
            vmem((HEADS, TOK), F32),
            vmem((TOK, 4 * CW), BF),
            vmem((TOK, 4 * CW), BF),
            vmem((CW, WIDTH), BF),
            vmem((TOK, MODEL // 2), BF),
            dma((21,)),
            dma((2,)),
            dma((12,)),
            dma((CHUNKS,)), dma((CHUNKS,)), dma((CHUNKS,)), dma((CHUNKS,)),
            dma((4,)),
            dma((2,)),
        ],
        compiler_params=pltpu.CompilerParams(
            collective_id=0, has_side_effects=True, vmem_limit_bytes=45 << 20
        ),
        name="decayed_backward",
    )(queries, keys, values, upstream, out_weight, gain, log_decay)
    out = jax.ShapeDtypeStruct((1, TOK, WIDTH), BF)
    return pl.pallas_call(
        finish,
        out_shape=(out, out, out),
        in_specs=[here] * 7,
        out_specs=[hbm] * 3,
        scratch_shapes=[rows_bf, rows_bf, dma((3,))],
        compiler_params=pltpu.CompilerParams(vmem_limit_bytes=24 << 20),
        name="finish",
    )(*kept)


def solution(mesh):
    torus = Mesh(
        mesh.devices.reshape(4, 4, 2, mesh.shape["tp"], mesh.shape["pp"]),
        ("seq_0", "seq_1", "seq_2", "tp", "pp"),
    )
    rows = P("pp", SEQ, "tp")
    placed = (rows, rows, rows, rows, P("pp", "tp", None), P("pp", "tp"), P("pp", "tp", SEQ))
    return jax.shard_map(
        local, mesh=torus, in_specs=placed, out_specs=(rows, rows, rows), check_vma=False
    )
```

```python
import jax
import jax.numpy as jnp
from jax import lax
from jax.experimental import pallas as pl
from jax.experimental.pallas import tpu as pltpu
from jax.sharding import Mesh
from jax.sharding import PartitionSpec as P

HEAD = 128
SEQ = ("seq_0", "seq_1", "seq_2")
MESH = pl.DeviceIdType.MESH
EPS = 1e-06
BF = jnp.bfloat16
F32 = jnp.float32

TOK = 512
HALF = 256
WIDTH = 2048
HEADS = 16
MODEL = 3072
CHUNKS = 12
CW = 128
BLOCKS = 32
ROWS = 64
FEATURES = 4096


def mark(name):
    pass


def nn(a, b):
    return lax.dot_general(a, b, (((1,), (0,)), ((), ())), preferred_element_type=F32)


def nt(a, b):
    return lax.dot_general(a, b, (((1,), (1,)), ((), ())), preferred_element_type=F32)


def lanes(h):
    return pl.ds(pl.multiple_of(h * HEAD, HEAD), HEAD)


def pair_lanes(i):
    if isinstance(i, int):
        return pl.ds(i * 2 * HEAD, 2 * HEAD)
    return pl.ds(pl.multiple_of(i * 2 * HEAD, 2 * HEAD), 2 * HEAD)


def two_states(ref, i):
    none = jnp.zeros((HEAD, HEAD), BF)
    first = jnp.concatenate([ref[4 * i], ref[4 * i + 1]], axis=0)
    second = jnp.concatenate([ref[4 * i + 2], ref[4 * i + 3]], axis=0)
    return jnp.concatenate(
        [jnp.concatenate([first, none], axis=1), jnp.concatenate([none, second], axis=1)], axis=0
    )


def two_columns(ref, i):
    return jnp.concatenate([ref[2 * i], ref[2 * i + 1]], axis=1)


def place(c, part):
    if c < CHUNKS - 2:
        return c // 2 * 4 * CW + part * 2 * CW + c % 2 * CW
    return (2 * c + part) * CW


def kernel(
    q_hbm, k_hbm, v_hbm, up_hbm, w_hbm, gain_hbm, ld_hbm,
    dqs, att, gh, k, v, later, tails,
    ccol, totals, q, w, up, ga, wqt, crow, mta, mtb,
    own_f, got_f, scan_f, state, own_b, got_b, scan_b,
    tot_in, sq_own, sq_in, cr_own, cr_in, inv, fac, gain, ld, b_own, b_in, w_last, up_from,
    load_sem, tot_sem, a2a_sem, perm_send, perm_recv, fwd_send, fwd_recv, tp_sem, b_sem,
):
    z, y, x = (lax.axis_index(a) for a in SEQ)
    me = z * 8 + y * 2 + x
    tp = lax.axis_index("tp")
    sibling = {"tp": 1 - tp}
    across = {"pp": 1 - lax.axis_index("pp")}

    zs = [lax.rem(z + d, 4) for d in range(4)]
    ys = [lax.rem(y + d, 4) for d in range(4)]
    xs = [x, 1 - x]
    def hops(at):
        return min(at[0], 4 - at[0]) + min(at[1], 4 - at[1]) + at[2]

    offsets = [(i, j, k) for i in range(4) for j in range(4) for k in range(2)][1:]
    offsets.sort(key=hops, reverse=True)

    def peer(at):
        i, j, k = at
        device = {"seq_0": zs[i], "seq_1": ys[j], "seq_2": xs[k]}
        return zs[i] * 8 + ys[j] * 2 + xs[k], device

    peers = [peer(at) for at in offsets]

    mark("loads")
    loads = []

    def load(src, dst):
        copy = pltpu.make_async_copy(src, dst, load_sem.at[len(loads)])
        copy.start()
        loads.append(copy)
        return copy

    first, rest = pl.ds(0, 2 * CW), pl.ds(2 * CW, MODEL // 2 - 2 * CW)
    up_loads = [load(up_hbm.at[0, :, cols], up_from.at[:, cols]) for cols in (first, rest)]
    ld_load = load(ld_hbm.at[0], ld)
    k_load = load(k_hbm.at[0], k)
    v_load = load(v_hbm.at[0], v)
    q_load = load(q_hbm.at[0], q)
    gain_load = load(gain_hbm, gain)
    w_loads = []
    for j in (0, 2, 4, 6, 8, 10, 11):
        wide = CW if j >= CHUNKS - 2 else 2 * CW
        for part, side in enumerate((tp, 1 - tp)):
            at = pl.multiple_of(side * (MODEL // 2) + j * CW, CW)
            w_loads.append(
                load(w_hbm.at[0, :, pl.ds(at, wide)], w.at[:, pl.ds(place(j, part), wide)])
            )

    mark("barrier")
    barrier = pltpu.get_barrier_semaphore()

    for _, device in peers:
        pl.semaphore_signal(barrier, inc=1, device_id=device, device_id_type=MESH)
    pl.semaphore_signal(barrier, inc=1, device_id=sibling, device_id_type=MESH)
    pl.semaphore_signal(barrier, inc=1, device_id=across, device_id_type=MESH)
    pl.semaphore_wait(barrier, BLOCKS + 1)

    def permute(j):
        return pltpu.make_async_remote_copy(
            src_ref=up_from.at[:, pl.ds(j * CW, CW)],
            dst_ref=up.at[:, pl.ds(place(j, 0), CW)],
            send_sem=perm_send.at[j],
            recv_sem=perm_recv.at[j],
            device_id=across,
            device_id_type=MESH,
        )

    def forward(j):
        return pltpu.make_async_remote_copy(
            src_ref=up.at[:, pl.ds(place(j, 0), CW)],
            dst_ref=up.at[:, pl.ds(place(j, 1), CW)],
            send_sem=fwd_send.at[j],
            recv_sem=fwd_recv.at[j],
            device_id=sibling,
            device_id_type=MESH,
        )

    def exchange(src, dst, send_sem, recv_sem):
        for p, device in peers:
            pltpu.make_async_remote_copy(
                src_ref=src.at[p],
                dst_ref=dst.at[me],
                send_sem=send_sem,
                recv_sem=recv_sem,
                device_id=device,
                device_id_type=MESH,
            ).start()
        dst[me] = src[me]

    def arrived(ref, sem):
        whole = ref.at[pl.ds(0, BLOCKS - 1)]
        pltpu.make_async_copy(whole, whole, sem).wait()

    mark("perm01")
    up_loads[0].wait()
    for j in (0, 1):
        permute(j).start()

    ld_load.wait()
    mark("cumsum")
    cum = ld[...]
    column_of = lax.broadcasted_iota(jnp.int32, (HEADS, TOK), 1)
    step = 1
    while step < TOK:
        moved = pltpu.roll(cum, step, 1)
        cum = cum + jnp.where(column_of >= step, moved, 0.0)
        step *= 2
    crow[...] = cum
    total = jnp.broadcast_to(cum[:, TOK - 1 : TOK], (HEADS, HEAD))
    for h in range(HEADS):
        totals[2 * h : 2 * h + 1, 0] = total[h : h + 1]
        totals[2 * h + 1 : 2 * h + 2, 0] = total[h : h + 1]
    mark("ccol")
    turned = cum.T
    for h in range(HEADS):
        ccol[h] = jnp.broadcast_to(turned[:, h : h + 1], (TOK, HEAD))

    mark("kvwait")
    k_load.wait()
    v_load.wait()

    mark("localstate")
    @pl.loop(0, HEADS, unroll=4)
    def _(h):
        tail = jnp.exp(totals[2 * h] - ccol[h])
        tails[h] = tail
        weighted = (k[:, lanes(h)].astype(F32) * tail).astype(BF)
        local_state = nn(weighted.T, v[:, lanes(h)]).astype(BF)
        own_f[2 * h] = local_state[:ROWS]
        own_f[2 * h + 1] = local_state[ROWS:]

    mark("a2a_f1_send")
    exchange(own_f, got_f, a2a_sem.at[0], a2a_sem.at[1])
    exchange(totals, tot_in, tot_sem.at[0], tot_sem.at[1])
    up_loads[1].wait()
    for j in (2, 3, 4):
        permute(j).start()
    q_load.wait()

    mark("intra")
    lower = lax.broadcasted_iota(jnp.int32, (HALF, HALF), 0) >= lax.broadcasted_iota(
        jnp.int32, (HALF, HALF), 1
    )
    upper = lax.broadcasted_iota(jnp.int32, (HALF, HALF), 0) <= lax.broadcasted_iota(
        jnp.int32, (HALF, HALF), 1
    )
    low = -1e30

    def decay_parts(h):
        col = ccol[h]
        col2 = jnp.concatenate([col, col], axis=1)
        row = crow[pl.ds(h, 1), :]
        c0, c1 = col2[:HALF], col2[HALF:]
        r0, r1 = row[:, :HALF], row[:, HALF:]
        d00 = jnp.exp(jnp.where(lower, c0 - r0, low))
        d10 = jnp.exp(c1 - r0)
        d11 = jnp.exp(jnp.where(lower, c1 - r1, low))
        return d00, d10, d11

    def turned_parts(h):
        col = ccol[h]
        col2 = jnp.concatenate([col, col], axis=1)
        row = crow[pl.ds(h, 1), :]
        c0, c1 = col2[:HALF], col2[HALF:]
        r0, r1 = row[:, :HALF], row[:, HALF:]
        t00 = jnp.exp(jnp.where(upper, r0 - c0, low))
        t01 = jnp.exp(r1 - c0)
        t11 = jnp.exp(jnp.where(upper, r1 - c1, low))
        return t00, t01, t11

    @pl.loop(0, HEADS)
    def _(h):
        qh, kh, vh = q[:, lanes(h)], k[:, lanes(h)], v[:, lanes(h)]
        q0, q1, k0, k1 = qh[:HALF], qh[HALF:], kh[:HALF], kh[HALF:]
        d00, d10, d11 = decay_parts(h)
        m00 = (nt(q0, k0) * d00).astype(BF)
        m10 = (nt(q1, k0) * d10).astype(BF)
        m11 = (nt(q1, k1) * d11).astype(BF)
        att[:HALF, lanes(h)] = nn(m00, vh[:HALF])
        att[HALF:, lanes(h)] = nn(jnp.concatenate([m10, m11], axis=1), vh)
        t00, t01, t11 = turned_parts(h)
        mta[h, :, :HALF] = (nt(k0, q0) * t00).astype(BF)
        mta[h, :, HALF:] = (nt(k0, q1) * t01).astype(BF)
        mtb[h] = (nt(k1, q1) * t11).astype(BF)
        wq = (qh.astype(F32) * jnp.exp(ccol[h])).astype(BF)
        wqt[h] = wq.T

    mark("wait_f1")
    arrived(tot_in, tot_sem.at[1])
    arrived(got_f, a2a_sem.at[1])
    mark("scan_f")
    running = jnp.zeros((ROWS, HEAD), F32)
    for b in range(BLOCKS):
        scan_f[b] = running.astype(BF)
        running = jnp.exp(tot_in[b]) * running + got_f[b].astype(F32)
    mark("a2a_f2_send")
    exchange(scan_f, state, a2a_sem.at[2], a2a_sem.at[3])
    for j in range(5, CHUNKS):
        permute(j).start()

    mark("wload")
    gain_load.wait()
    for copy in w_loads:
        copy.wait()

    def hidden(start, depth, first):
        @pl.loop(0, 4, unroll=2)
        def _(n):
            at = pl.ds(pl.multiple_of(n * 512, 512), 512)
            part = nt(up[:, start : start + depth], w[at, start : start + depth])
            if first:
                gh[:, at] = part
            else:
                gh[:, at] += part

    def relay(*chunks):
        for j in chunks:
            permute(j).wait_recv()
            forward(j).start()

    def relayed(*chunks):
        for j in chunks:
            forward(j).wait_recv()

    @pl.loop(0, HEADS, unroll=2)
    def _(h):
        turned = w[lanes(h), MODEL - CW :].astype(F32).T
        w_last[:, lanes(h)] = (turned * gain[:, lanes(h)]).astype(BF)

    mark("relay012")
    relay(0, 1, 2, 3)
    relayed(0, 1)
    mark("hidden01")
    hidden(0, 512, True)
    mark("relay23")
    relay(4)
    relayed(2, 3)
    mark("hidden23")
    hidden(512, 512, False)

    mark("wait_f2")
    arrived(state, a2a_sem.at[3])
    mark("att_inter")
    sq_own[...] = jnp.zeros_like(sq_own)

    @pl.loop(0, HEADS // 2, unroll=2)
    def _(i):
        at = pair_lanes(i)
        new = att[:, at] + jnp.exp(two_columns(ccol, i)) * nn(q[:, at], two_states(state, i))
        att[:, at] = new
        ga[:, at] = (new * gain[:, at]).astype(BF)
        both = new * new
        sq_own[...] += both[:, :HEAD] + both[:, HEAD:]

    def to_sibling(src, dst, i):
        return pltpu.make_async_remote_copy(
            src_ref=src,
            dst_ref=dst,
            send_sem=tp_sem.at[2 * i],
            recv_sem=tp_sem.at[2 * i + 1],
            device_id=sibling,
            device_id_type=MESH,
        )

    def tail_product():
        b_own[...] = nn(ga[...], w[:, 2560:]).astype(BF)
        for at in range(0, 4 * CW, CW):
            copy = pltpu.make_async_remote_copy(
                src_ref=b_own.at[:, pl.ds(at, CW)],
                dst_ref=b_in.at[:, pl.ds(at + CW if at % (2 * CW) == 0 else at - CW, CW)],
                send_sem=b_sem.at[0],
                recv_sem=b_sem.at[1],
                device_id=sibling,
                device_id_type=MESH,
            )
            copy.start()

    squares = to_sibling(sq_own, sq_in, 0)
    squares.start()
    cr_own[...] = jnp.zeros_like(cr_own)
    mark("tail_product")
    tail_product()
    mark("relay45")
    relay(5)
    relayed(4, 5)
    mark("hidden45")
    hidden(1024, 512, False)
    mark("inverse")
    squares.wait_recv()
    square_total = jnp.sum(sq_own[...] + sq_in[...], axis=1, keepdims=True)
    inv[...] = jnp.broadcast_to(1.0 / jnp.sqrt(square_total / FEATURES + EPS), (TOK, HEAD))
    mark("relay67")
    relay(6, 7)
    relayed(6, 7)
    mark("hidden67")
    hidden(1536, 512, False)
    mark("relay89")
    relay(8, 9)
    relayed(8, 9)
    mark("hidden89")

    @pl.loop(0, 4, unroll=2)
    def _(n):
        at = pl.ds(pl.multiple_of(n * 512, 512), 512)
        new = gh[:, at] + nt(up[:, 2048:2560], w[at, 2048:2560])
        gh[:, at] = new
        both = new * gain[:, at] * att[:, at]
        cr_own[...] += (both[:, :128] + both[:, 128:256]) + (both[:, 256:384] + both[:, 384:])

    crossed = to_sibling(cr_own, cr_in, 1)
    crossed.start()
    mark("relay10")
    relay(10)
    mark("own10")
    hidden(2560, 128, False)
    pltpu.make_async_copy(b_in, b_in, b_sem.at[1]).wait()
    crossed.wait_recv()
    mark("relay11")
    relay(11)
    relayed(10)
    mark("sib10own11")

    @pl.loop(0, 4, unroll=2)
    def _(n):
        at = pl.ds(pl.multiple_of(n * 512, 512), 512)
        new = gh[:, at] + nt(up[:, 2688:2944], w[at, 2688:2944])
        inverse = inv[...]
        gh[:, at] = new * gain[:, at] * jnp.concatenate([inverse] * 4, axis=1)

    crossed.wait_send()
    part = cr_own[...] + cr_in[...]
    for at in range(0, 3 * CW, CW):
        both = b_own[:, at : at + CW].astype(F32) + b_in[:, at : at + CW].astype(F32)
        part += up[:, 2560 + at : 2560 + at + CW].astype(F32) * both
    cr_own[...] = part
    mark("relayed11")
    relayed(11)
    mark("crossing11")
    both = b_own[:, 3 * CW :].astype(F32) + b_in[:, 3 * CW :].astype(F32)
    part = cr_own[...] + up[:, MODEL - CW :].astype(F32) * both
    cross_total = jnp.sum(part, axis=1, keepdims=True)
    inverse = inv[...]
    fac[...] = inverse * inverse * inverse * jnp.broadcast_to(cross_total / FEATURES, (TOK, HEAD))
    up_last = (up[:, MODEL - CW :].astype(F32) * inverse).astype(BF)

    mark("ga_passed")
    low_rows, high_rows = pl.ds(0, ROWS // 2), pl.ds(ROWS // 2, ROWS // 2)

    def send_piece(src, dst, p, device, rows, sem):
        pltpu.make_async_remote_copy(
            src_ref=src.at[p, rows],
            dst_ref=dst.at[me, rows],
            send_sem=a2a_sem.at[sem],
            recv_sem=a2a_sem.at[sem + 1],
            device_id=device,
            device_id_type=MESH,
        ).start()

    def piece_arrived(ref, rows, sem):
        whole = ref.at[pl.ds(0, BLOCKS - 1), rows]
        pltpu.make_async_copy(whole, whole, a2a_sem.at[sem]).wait()

    def passing(i):
        at = pair_lanes(i)
        both = gh[:, at] + nn(up_last, w_last[:, at])
        factor = fac[...]
        both = both - jnp.concatenate([factor, factor], axis=1) * att[:, at]
        both = both.astype(BF)
        ga[:, at] = both
        for side in (0, 1):
            h = 2 * i + side
            passed = nn(wqt[h], both[:, side * HEAD : (side + 1) * HEAD]).astype(BF)
            own_b[2 * h] = passed[:ROWS]
            own_b[2 * h + 1] = passed[ROWS:]

    for group in ((2, 1), (3, 0)):
        for n in group:
            passing(2 * zs[n])
            passing(2 * zs[n] + 1)
        for p, device in (peer(at) for at in offsets if at[0] in group):
            send_piece(own_b, got_b, p, device, low_rows, 4)
    mark("send_high")
    for p, device in peers:
        send_piece(own_b, got_b, p, device, high_rows, 6)
    got_b[me] = own_b[me]

    def gradients(i):
        two = pair_lanes(i)
        inter = jnp.exp(two_columns(ccol, i)) * nt(ga[:, two], two_states(state, i))
        for side in (0, 1):
            h = 2 * i + side
            qh, kh, vh, gah = q[:, lanes(h)], k[:, lanes(h)], v[:, lanes(h)], ga[:, lanes(h)]
            v0, v1, g0, g1 = vh[:HALF], vh[HALF:], gah[:HALF], gah[HALF:]
            d00, d10, d11 = decay_parts(h)
            m00 = (nt(g0, v0) * d00).astype(BF)
            m10 = (nt(g1, v0) * d10).astype(BF)
            m11 = (nt(g1, v1) * d11).astype(BF)
            dq0 = nn(m00, kh[:HALF])
            dq1 = nn(jnp.concatenate([m10, m11], axis=1), kh)
            more = inter[:, side * HEAD : (side + 1) * HEAD]
            dqs[:HALF, lanes(h)] = (dq0 + more[:HALF]).astype(BF)
            dqs[HALF:, lanes(h)] = (dq1 + more[HALF:]).astype(BF)
            att[:HALF, lanes(h)] = nn(jnp.concatenate([m00.T, m10.T], axis=1), qh)
            att[HALF:, lanes(h)] = nn(m11.T, qh[HALF:])
            gh[:HALF, lanes(h)] = nn(mta[h], gah)
            gh[HALF:, lanes(h)] = nn(mtb[h], g1)

    def scan_back(rows):
        running = jnp.zeros((ROWS // 2, HEAD), F32)
        for b in reversed(range(BLOCKS)):
            scan_b[b, rows] = running.astype(BF)
            running = jnp.exp(tot_in[b]) * running + got_b[b, rows].astype(F32)
        for p, device in peers:
            send_piece(scan_b, later, p, device, rows, 8 if rows is low_rows else 10)
        later[me, rows] = scan_b[me, rows]

    mark("grad1")
    pl.loop(0, 3)(gradients)
    mark("wait_b1a")
    piece_arrived(got_b, low_rows, 5)
    mark("scan_ba")
    scan_back(low_rows)
    mark("grad2")
    pl.loop(3, 4)(gradients)
    mark("wait_b1b")
    piece_arrived(got_b, high_rows, 7)
    mark("scan_bb")
    scan_back(high_rows)
    mark("grad3")
    pl.loop(4, HEADS // 2)(gradients)
    mark("wait_b2")
    piece_arrived(later, low_rows, 9)
    piece_arrived(later, high_rows, 11)

    mark("sendwaits")
    arrived(totals, tot_sem.at[0])
    arrived(own_f, a2a_sem.at[0])
    arrived(scan_f, a2a_sem.at[2])
    for rows, sem in ((low_rows, 4), (high_rows, 6)):
        piece_arrived(own_b, rows, sem)
        piece_arrived(scan_b, rows, sem + 4)
    pltpu.make_async_copy(b_own, b_own, b_sem.at[0]).wait()
    for j in range(CHUNKS):
        permute(j).wait_send()
        forward(j).wait_send()
    squares.wait_send()
    mark(None)


def finish(
    dqs, att, gh, k, v, later, tails, dq_hbm, dk_hbm, dv_hbm, dks, dvs, out_sem
):
    pltpu.make_async_copy(dqs, dq_hbm.at[0], out_sem.at[0]).start()

    def put(src, dst, at, i):
        pltpu.make_async_copy(src.at[:, at], dst.at[0, :, at], out_sem.at[i]).start()

    for i in range(HEADS // 2):
        at = pair_lanes(i)
        lt = two_states(later, i)
        tail = two_columns(tails, i)
        dks[:, at] = (att[:, at] + tail * nt(v[:, at], lt)).astype(BF)
        dvs[:, at] = (gh[:, at] + tail * nn(k[:, at], lt)).astype(BF)
        if i % 2 == 1:
            part = pl.ds((i - 1) * 2 * HEAD, 4 * HEAD)
            put(dks, dk_hbm, part, 1)
            put(dvs, dv_hbm, part, 2)

    for i, (src, dst) in enumerate(((dqs, dq_hbm), (dks, dk_hbm), (dvs, dv_hbm))):
        pltpu.make_async_copy(src, dst.at[0], out_sem.at[i]).wait()


def local(queries, keys, values, upstream, out_weight, gain, log_decay):
    vmem = pltpu.VMEM
    piece = vmem((BLOCKS, ROWS, HEAD), BF)
    column = vmem((TOK, HEAD), F32)
    rows_bf = vmem((TOK, WIDTH), BF)
    rows_f32 = vmem((TOK, WIDTH), F32)
    columns = vmem((HEADS, TOK, HEAD), F32)
    totals = vmem((BLOCKS, 1, HEAD), F32)
    dma = pltpu.SemaphoreType.DMA
    hbm = pl.BlockSpec(memory_space=pl.ANY)
    here = pl.BlockSpec(memory_space=vmem)
    kept = pl.pallas_call(
        kernel,
        out_shape=(rows_bf, rows_f32, rows_f32, rows_bf, rows_bf, piece, columns),
        in_specs=[hbm] * 7,
        out_specs=[here] * 7,
        scratch_shapes=[
            columns,
            totals,
            rows_bf,
            vmem((WIDTH, MODEL), BF),
            vmem((TOK, MODEL), BF),
            rows_bf,
            vmem((HEADS, HEAD, TOK), BF),
            vmem((HEADS, TOK), F32),
            vmem((HEADS, HALF, TOK), BF),
            vmem((HEADS, HALF, HALF), BF),
            piece, piece, piece, piece, piece, piece, piece,
            totals,
            column, column, column, column, column, column,
            vmem((1, WIDTH), F32),
            vmem((HEADS, TOK), F32),
            vmem((TOK, 4 * CW), BF),
            vmem((TOK, 4 * CW), BF),
            vmem((CW, WIDTH), BF),
            vmem((TOK, MODEL // 2), BF),
            dma((21,)),
            dma((2,)),
            dma((12,)),
            dma((CHUNKS,)), dma((CHUNKS,)), dma((CHUNKS,)), dma((CHUNKS,)),
            dma((4,)),
            dma((2,)),
        ],
        compiler_params=pltpu.CompilerParams(
            collective_id=0, has_side_effects=True, vmem_limit_bytes=45 << 20
        ),
        name="decayed_backward",
    )(queries, keys, values, upstream, out_weight, gain, log_decay)
    out = jax.ShapeDtypeStruct((1, TOK, WIDTH), BF)
    return pl.pallas_call(
        finish,
        out_shape=(out, out, out),
        in_specs=[here] * 7,
        out_specs=[hbm] * 3,
        scratch_shapes=[rows_bf, rows_bf, dma((3,))],
        compiler_params=pltpu.CompilerParams(vmem_limit_bytes=24 << 20),
        name="finish",
    )(*kept)


def solution(mesh):
    torus = Mesh(
        mesh.devices.reshape(4, 4, 2, mesh.shape["tp"], mesh.shape["pp"]),
        ("seq_0", "seq_1", "seq_2", "tp", "pp"),
    )
    rows = P("pp", SEQ, "tp")
    placed = (rows, rows, rows, rows, P("pp", "tp", None), P("pp", "tp"), P("pp", "tp", SEQ))
    return jax.shard_map(
        local, mesh=torus, in_specs=placed, out_specs=(rows, rows, rows), check_vma=False
    )
```
